32 devices in a mesh: pool: 2 (over x), seq: 4 (over y, core), head: 4 (over z).
Axes of the slice: x: 2, y: 2, z: 4, core: 2. Of those that a mesh axis runs over, the one named last changes fastest.
Arguments:
- prompt: bfloat16 [8, 2048, 8192], P('pool', 'seq'), may hold values from -6 to 6
- key_value_weight: bfloat16 [8192, 2, 1024], P('seq', None, 'head'), may hold values from -0.0625 to 0.0625
- adapter_down_weight: bfloat16 [8192, 256], P('seq'), may hold values from -0.0625 to 0.0625
- adapter_up_weight: bfloat16 [8, 2, 16, 1024], P(None, None, None, 'head'), may hold values from -0.75 to 0.75
- request_adapter_index: int32 [8], P('pool'), may hold values from 0 to 7
- destination: int32 [8], replicated, may hold values from 0 to 3, as said below
- rotated_query: bfloat16 [384, 8192], P(('pool', 'seq'), 'head'), may hold values from -150 to 150
- key_value_cache: bfloat16 [384, 128, 2, 1024], P(('pool', 'seq'), None, None, 'head'), may hold values from -6 to 6
- current_key_value: bfloat16 [384, 2, 1024], P(('pool', 'seq'), None, 'head'), may hold values from -6 to 6
- cached_length: int32 [384], P(('pool', 'seq')), may hold values from 1 to 128
- row_adapter_index: int32 [384], P('pool'), may hold values from 0 to 7
- output_weight: bfloat16 [8192, 8192], P('head', 'seq'), may hold values from -0.0625 to 0.0625
- output_down_weight: bfloat16 [8192, 8, 16], P('head'), may hold values from -0.0625 to 0.0625
- output_up_weight: bfloat16 [8, 16, 8192], P(None, None, 'seq'), may hold values from -3.59375 to 3.59375
Outputs:
- handed: bfloat16 [8, 2, 2048, 2, 1024], P(('pool', 'seq'), None, None, None, 'head')
- decoded: bfloat16 [384, 8192], P(('pool', 'head'), 'seq')
The draws below stay inside these ranges and needn't reach their ends.
Inputs may be any that keep to these rules, and one draw needn't show every extreme that they name: `destination`: among one pool's 4 requests no decode owner is named more than 2 times, and some owner exactly 2 times; in each pool owners 0 and 3 both receive requests.
All inputs are finite; a program needn't handle non-finite values.
Results may differ from the reference program's by a relative error of at most 0.0085.
Values may be sent and summed in bfloat16 or wider, within the bound.
A program may use at most 128 MiB of HBM per device.

```python
import jax
import jax.numpy as jnp
from jax import lax

MODEL_DIM = 8192
QUERY_HEADS = 64
KEY_HEADS = 8
HEAD_DIM = 128
ADAPTER_RANK = 16
ADAPTER_COUNT = 8
PROMPT = 2048
CAP = 2
REQ_POOL = 4
ROWS_DEV = 48
CONTEXT_SLOTS = 128
REQS = 8
DECODE_ROWS = 384
DECODERS = 4
OWNERS = 8
N_POOL = 2
N_SEQ = 4


def cache_front(key):
    leading_part = jax.random.normal(jax.random.fold_in(key, 11), (DECODE_ROWS, 2, 2, KEY_HEADS * HEAD_DIM), jnp.float32)
    leading_part = jnp.clip(leading_part, -6.0, 6.0)
    return leading_part


def draw_key_value_cache(key, part):
    leading_part = cache_front(key)
    remaining_part = jax.random.normal(jax.random.fold_in(key, 12), (DECODE_ROWS, CONTEXT_SLOTS - 2, 2, KEY_HEADS * HEAD_DIM), jnp.float32)
    remaining_part = jnp.clip(remaining_part, -6.0, 6.0)
    whole = jnp.concatenate([leading_part, remaining_part], axis=1)
    return jnp.clip(whole, -6.0, 6.0).astype(jnp.bfloat16)


def draw_rotated_query(key, part):
    query_matrix = jax.random.normal(jax.random.fold_in(key, 21), (DECODE_ROWS, QUERY_HEADS * HEAD_DIM), jnp.float32)
    query_matrix = jnp.clip(query_matrix, -5.0, 5.0)
    return query_matrix.astype(jnp.bfloat16)


def draw_destination(key, part):
    halves = []
    for pool_index in range(N_POOL):
        sub_key = jax.random.fold_in(key, 100 + pool_index)
        ranks = jax.random.permutation(jax.random.fold_in(sub_key, 1), N_SEQ).astype(jnp.int32)
        coin = jax.random.randint(jax.random.fold_in(sub_key, 4), (), 0, 2).astype(jnp.int32)
        first_owner = coin * (N_SEQ - 1)
        second_owner = N_SEQ - 1 - first_owner
        ranks = ranks.at[first_owner].set(-2)
        ranks = ranks.at[second_owner].set(-1)
        owners = jnp.argsort(ranks, stable=True).astype(jnp.int32)
        counts = jax.random.randint(jax.random.fold_in(sub_key, 2), (N_SEQ,), 1, CAP + 1)
        counts = counts.at[0].set(CAP)
        listed = jnp.repeat(owners, counts, total_repeat_length=REQ_POOL)
        shuffle = jax.random.permutation(jax.random.fold_in(sub_key, 3), REQ_POOL)
        halves.append(listed[shuffle])
    return jnp.concatenate(halves).astype(jnp.int32)


def place_ends(values, key, smallest, top_value):
    index_at = [jax.random.randint(jax.random.fold_in(key, axis), (), 0, length) for axis, length in enumerate(values.shape)]
    widest = values.shape.index(max(values.shape))
    beside = index_at[:widest] + [(index_at[widest] + 1) % values.shape[widest]] + index_at[widest + 1:]
    return values.at[tuple(index_at)].set(smallest).at[tuple(beside)].set(top_value)


def level_of(rng, dims, pieces, low, largest):
    level = 1.0
    for dim, blocks in pieces:
        heights = jax.random.uniform(jax.random.fold_in(jax.random.fold_in(rng, 6), dim), (blocks,), jnp.float32, low / len(pieces), largest / len(pieces))
        level = level * jnp.repeat(jnp.exp(heights), dims[dim] // blocks).reshape((-1,) + (1,) * (len(dims) - 1 - dim))
    return level


def noise(stream_key, dims, scale, reach, cuts=(), kind=jnp.bfloat16):
    values = jax.random.normal(stream_key, dims, jnp.float32) * scale
    if len(cuts) > 0:
        values = level_of(stream_key, dims, cuts, -0.22, 0.18) * values
    return jnp.clip(values, min=-reach, max=reach).astype(kind)


def setup_inputs(seed: int = 0) -> dict:
    key_of = jax.random.split(jax.random.key(seed), 15)
    prompt = noise(key_of[0], (REQS, PROMPT, MODEL_DIM), 1.0, 6.0, ((0, 2), (1, 4)))
    key_value_weight = noise(key_of[1], (MODEL_DIM, 2, KEY_HEADS * HEAD_DIM), MODEL_DIM ** -0.5, 0.0625, ((0, 4), (2, 4)))
    adapter_down_weight = noise(key_of[2], (MODEL_DIM, ADAPTER_COUNT * 2 * ADAPTER_RANK), MODEL_DIM ** -0.5, 0.0625, ((0, 4),))
    adapter_up_weight = noise(key_of[3], (ADAPTER_COUNT, 2, ADAPTER_RANK, KEY_HEADS * HEAD_DIM), 0.125, 0.75, ((3, 4),))
    request_adapter_index = place_ends(jax.random.randint(key_of[4], (REQS,), 0, ADAPTER_COUNT), jax.random.fold_in(key_of[4], 1), 0, ADAPTER_COUNT - 1).astype(jnp.int32)
    destination = draw_destination(jax.random.fold_in(key_of[14], 71), 0)
    rotated_query = draw_rotated_query(jax.random.fold_in(key_of[14], 71), 0)
    key_value_cache = draw_key_value_cache(jax.random.fold_in(key_of[14], 71), 0)
    current_key_value = noise(key_of[8], (DECODE_ROWS, 2, KEY_HEADS * HEAD_DIM), 1.0, 6.0, ((0, 8), (2, 4)))
    cached_length = place_ends(jax.random.randint(key_of[9], (DECODE_ROWS,), 1, CONTEXT_SLOTS + 1), jax.random.fold_in(key_of[9], 1), 1, CONTEXT_SLOTS).astype(jnp.int32)
    row_adapter_index = place_ends(jax.random.randint(key_of[10], (DECODE_ROWS,), 0, ADAPTER_COUNT), jax.random.fold_in(key_of[10], 1), 0, ADAPTER_COUNT - 1).astype(jnp.int32)
    output_weight = noise(key_of[11], (QUERY_HEADS * HEAD_DIM, MODEL_DIM), (QUERY_HEADS * HEAD_DIM) ** -0.5, 0.0625, ((0, 4), (1, 4)))
    output_down_weight = noise(key_of[12], (QUERY_HEADS * HEAD_DIM, ADAPTER_COUNT, ADAPTER_RANK), (QUERY_HEADS * HEAD_DIM) ** -0.5, 0.0625, ((0, 4),))
    output_up_weight = noise(key_of[13], (ADAPTER_COUNT, ADAPTER_RANK, MODEL_DIM), 0.6, 3.59375, ((2, 4),))
    return {"prompt": prompt, "key_value_weight": key_value_weight, "adapter_down_weight": adapter_down_weight, "adapter_up_weight": adapter_up_weight, "request_adapter_index": request_adapter_index, "destination": destination, "rotated_query": rotated_query, "key_value_cache": key_value_cache, "current_key_value": current_key_value, "cached_length": cached_length, "row_adapter_index": row_adapter_index, "output_weight": output_weight, "output_down_weight": output_down_weight, "output_up_weight": output_up_weight}


def attend_rows(query_matrix, key_value_cache, prefill_state, lengths):
    decode_count = query_matrix.shape[0]
    query_groups = QUERY_HEADS // KEY_HEADS
    query_batch = query_matrix.astype(jnp.float32).reshape(decode_count, KEY_HEADS, query_groups, HEAD_DIM)
    key_matrix = key_value_cache[:, :, 0].astype(jnp.float32).reshape(decode_count, CONTEXT_SLOTS, KEY_HEADS, HEAD_DIM)
    value_matrix = key_value_cache[:, :, 1].astype(jnp.float32).reshape(decode_count, CONTEXT_SLOTS, KEY_HEADS, HEAD_DIM)
    prefill_key = prefill_state[:, 0].astype(jnp.float32).reshape(decode_count, KEY_HEADS, HEAD_DIM)
    prefill_value = prefill_state[:, 1].astype(jnp.float32).reshape(decode_count, KEY_HEADS, HEAD_DIM)
    factor = HEAD_DIM ** -0.5
    scores = jnp.einsum("rkgd,rckd->rkgc", query_batch, key_matrix) * factor
    own_score = jnp.einsum("rkgd,rkd->rkg", query_batch, prefill_key) * factor
    valid = (jnp.arange(CONTEXT_SLOTS, dtype=jnp.int32)[None, :] < lengths[:, None])[:, None, None, :]
    highest = jnp.maximum(jnp.max(jnp.where(valid, scores, -1e30), axis=-1), own_score)
    raw = jnp.where(valid, jnp.exp(scores - highest[..., None]), 0.0)
    own_raw = jnp.exp(own_score - highest)
    normer = jnp.sum(raw, axis=-1) + own_raw
    weights = lax.optimization_barrier((raw / normer[..., None]).astype(jnp.bfloat16)).astype(jnp.float32)
    own_weight = lax.optimization_barrier((own_raw / normer).astype(jnp.bfloat16)).astype(jnp.float32)
    mixed = jnp.einsum("rkgc,rckd->rkgd", weights, value_matrix)
    mixed = mixed + own_weight[..., None] * prefill_value[:, :, None, :]
    return mixed.reshape(decode_count, QUERY_HEADS * HEAD_DIM).astype(jnp.bfloat16)


def reference(prompt, key_value_weight, adapter_down_weight, adapter_up_weight, request_adapter_index, destination, rotated_query, key_value_cache, current_key_value, cached_length, row_adapter_index, output_weight, output_down_weight, output_up_weight):
    key_value_width = KEY_HEADS * HEAD_DIM
    token_matrix = prompt.reshape(REQS * PROMPT, MODEL_DIM)
    base_kv = jnp.dot(token_matrix, key_value_weight.reshape(MODEL_DIM, 2 * key_value_width), preferred_element_type=jnp.float32)
    reduced_everything = jnp.dot(token_matrix, adapter_down_weight, preferred_element_type=jnp.float32)
    reduced_everything = reduced_everything.reshape(REQS, PROMPT, ADAPTER_COUNT, 2, ADAPTER_RANK)
    adapter_selector = request_adapter_index[:, None] == jnp.arange(ADAPTER_COUNT, dtype=jnp.int32)[None, :]
    low_rank = jnp.sum(jnp.where(adapter_selector[:, None, :, None, None], reduced_everything, 0.0), axis=2)
    selected_up_weight = adapter_up_weight.astype(jnp.float32)[request_adapter_index]
    correction = jnp.einsum("rtkq,rkqf->rtkf", low_rank, selected_up_weight, precision=lax.Precision.HIGHEST)
    prefilled = (base_kv.reshape(REQS, PROMPT, 2, key_value_width) + correction).astype(jnp.bfloat16)

    owners = destination.reshape(N_POOL, REQ_POOL)
    order_index = jnp.arange(REQ_POOL, dtype=jnp.int32)
    earlier = (owners[:, :, None] == owners[:, None, :]) & (order_index[None, None, :] < order_index[None, :, None])
    slot_of = jnp.sum(earlier.astype(jnp.int32), axis=2).astype(jnp.int32)
    target_pool = (jnp.arange(N_POOL, dtype=jnp.int32) + 1) % N_POOL
    target = (target_pool[:, None] * DECODERS + owners).reshape(REQS).astype(jnp.int32)
    handed = jnp.zeros((OWNERS, CAP, PROMPT, 2, key_value_width), jnp.bfloat16)
    handed = handed.at[target, slot_of.reshape(REQS)].set(prefilled)

    blocks = DECODE_ROWS // ROWS_DEV

    def one_block(operands):
        return attend_rows(operands[0], operands[1], operands[2], operands[3])

    attended = lax.map(one_block, (rotated_query.reshape(blocks, ROWS_DEV, QUERY_HEADS * HEAD_DIM), key_value_cache.reshape(blocks, ROWS_DEV, CONTEXT_SLOTS, 2, key_value_width), current_key_value.reshape(blocks, ROWS_DEV, 2, key_value_width), cached_length.reshape(blocks, ROWS_DEV)))
    attended = attended.reshape(DECODE_ROWS, QUERY_HEADS * HEAD_DIM)
    low_rows = jnp.dot(attended, output_down_weight.reshape(QUERY_HEADS * HEAD_DIM, ADAPTER_COUNT * ADAPTER_RANK), preferred_element_type=jnp.float32)
    keep = row_adapter_index[:, None] == (jnp.arange(ADAPTER_COUNT * ADAPTER_RANK, dtype=jnp.int32) // ADAPTER_RANK)[None, :]
    low_rows = jnp.where(keep, low_rows, 0.0)
    decoded = jnp.dot(attended, output_weight, preferred_element_type=jnp.float32)
    decoded = decoded + jnp.dot(low_rows, output_up_weight.reshape(ADAPTER_COUNT * ADAPTER_RANK, MODEL_DIM).astype(jnp.float32), precision=lax.Precision.HIGHEST)
    return handed, decoded.astype(jnp.bfloat16)
```

```python
import jax
import jax.numpy as jnp
from jax import lax
from jax.experimental import pallas as pl
from jax.experimental.pallas import tpu as pltpu
from jax.sharding import PartitionSpec as P

HEAD_DIM = 128
ADAPTER_RANK = 16
ADAPTER_COUNT = 8
CAP = 2


def exchanged(value, axis, mask):
    pairs = [(source, source ^ mask) for source in range(lax.axis_size(axis))]
    return lax.ppermute(value, axis, pairs)


def gathered(value, axis, after=None):
    size = lax.axis_size(axis)
    index = lax.axis_index(axis)
    held = value[None]
    mask = size // 2
    arrived = None
    while mask >= 1:
        other = exchanged(held, axis, mask)
        if after is not None:
            other = lax.optimization_barrier((other, after))[0]
        arrived = other if arrived is None else arrived
        low_bit = (index // mask) % 2 == 0
        first = jnp.where(low_bit, held, other)
        second = jnp.where(low_bit, other, held)
        held = jnp.stack([first, second], axis=1).reshape((-1,) + value.shape)
        mask //= 2
    return held, arrived


def scattered_sum(value, axis):
    size = lax.axis_size(axis)
    index = lax.axis_index(axis)
    held = value.reshape((size, value.shape[0] // size) + value.shape[1:])
    mask = 1
    while mask < size:
        split = held.reshape((held.shape[0] // 2, 2) + held.shape[1:])
        low_bit = (index // mask) % 2 == 0
        keep = jnp.where(low_bit, split[:, 0], split[:, 1])
        give = jnp.where(low_bit, split[:, 1], split[:, 0])
        held = keep + exchanged(give, axis, mask)
        mask *= 2
    return held[0]


def attend_kernel(lengths, query_ref, cache_ref, key_ref, value_ref, out_ref):
    rows, positions = cache_ref.shape[0], cache_ref.shape[1]
    kv_heads = key_ref.shape[1]
    groups = query_ref.shape[1] // kv_heads
    start = pl.program_id(0) * rows
    lane = lax.broadcasted_iota(jnp.int32, (groups, 2 * positions), 1)
    factor = HEAD_DIM ** (-0.5)
    blocks, scores, owns = [], [], []
    for row in range(rows):
        pairs = cache_ref[row].reshape(2 * positions, kv_heads * HEAD_DIM)
        valid = (lane % 2 == 0) & (lane < 2 * lengths[start + row])
        for head in range(kv_heads):
            block = pairs[:, head * HEAD_DIM : (head + 1) * HEAD_DIM]
            query = query_ref[row, head * groups : (head + 1) * groups, :]
            own_key = key_ref[row, head : head + 1, :].astype(jnp.float32)
            own = jnp.sum(query.astype(jnp.float32) * own_key, axis=1, keepdims=True) * factor
            score = lax.dot_general(
                query, block, (((1,), (1,)), ((), ())), preferred_element_type=jnp.float32
            )
            blocks.append(block)
            scores.append(jnp.where(valid, score * factor, -1e30))
            owns.append(own)
    scores = jnp.concatenate(scores, axis=0)
    own = jnp.concatenate(owns, axis=0)
    highest = jnp.maximum(jnp.max(scores, axis=1, keepdims=True), own)
    raw = jnp.where(scores > -1e29, jnp.exp(scores - highest), 0.0)
    own_raw = jnp.exp(own - highest)
    total = jnp.sum(raw, axis=1, keepdims=True) + own_raw
    weights = pltpu.roll(raw / total, 1, 1).astype(jnp.bfloat16)
    own_weight = (own_raw / total).astype(jnp.bfloat16).astype(jnp.float32)
    for row in range(rows):
        for head in range(kv_heads):
            at = (row * kv_heads + head) * groups
            own_value = value_ref[row, head : head + 1, :].astype(jnp.float32)
            mixed = jnp.dot(
                weights[at : at + groups],
                blocks[row * kv_heads + head],
                preferred_element_type=jnp.float32,
            )
            out_ref[row, head * groups : (head + 1) * groups, :] = (
                mixed + own_weight[at : at + groups] * own_value
            ).astype(jnp.bfloat16)


def attend(query, cache, current, lengths):
    rows, positions, _, width = cache.shape
    kv_heads = width // HEAD_DIM
    heads = query.shape[1] // HEAD_DIM
    step = next(size for size in (8, 4, 2, 1) if rows % size == 0)
    query = query.reshape(rows, heads, HEAD_DIM)
    own_key = current[:, 0].reshape(rows, kv_heads, HEAD_DIM)
    own_value = current[:, 1].reshape(rows, kv_heads, HEAD_DIM)
    out = pl.pallas_call(
        attend_kernel,
        grid_spec=pltpu.PrefetchScalarGridSpec(
            num_scalar_prefetch=1,
            grid=(rows // step,),
            in_specs=[
                pl.BlockSpec((step, heads, HEAD_DIM), lambda i, _: (i, 0, 0)),
                pl.BlockSpec((step, positions, 2, width), lambda i, _: (i, 0, 0, 0)),
                pl.BlockSpec((step, kv_heads, HEAD_DIM), lambda i, _: (i, 0, 0)),
                pl.BlockSpec((step, kv_heads, HEAD_DIM), lambda i, _: (i, 0, 0)),
            ],
            out_specs=pl.BlockSpec((step, heads, HEAD_DIM), lambda i, _: (i, 0, 0)),
        ),
        out_shape=jax.ShapeDtypeStruct((rows, heads, HEAD_DIM), jnp.bfloat16),
        cost_estimate=pl.CostEstimate(
            flops=8 * rows * heads * positions * HEAD_DIM,
            bytes_accessed=4 * rows * positions * width,
            transcendentals=2 * rows * heads * positions,
        ),
    )(lengths, query, cache, own_key, own_value)
    return out.reshape(rows, heads * HEAD_DIM)


def weave_kernel(key_ref, value_ref, out_ref):
    tokens, width = key_ref.shape[2], key_ref.shape[3]
    part = 128
    row = lax.broadcasted_iota(jnp.int32, (2 * part, 2 * part), 0)
    column = lax.broadcasted_iota(jnp.int32, (2 * part, 2 * part), 1)
    order = jnp.where(column == (row % 2) * part + row // 2, 1.0, 0.0).astype(jnp.bfloat16)
    for at in range(0, tokens, part):
        both = jnp.concatenate(
            [key_ref[0, 0, at : at + part, :], value_ref[0, 0, at : at + part, :]], axis=0
        )
        woven = jnp.dot(order, both, preferred_element_type=jnp.float32).astype(jnp.bfloat16)
        out_ref[0, 0, at : at + part, :, :] = woven.reshape(part, 2, width)


def weave(keys, values):
    sources, slots, tokens, width = keys.shape
    spec = pl.BlockSpec((1, 1, tokens, width), lambda slot, source: (source, slot, 0, 0))
    return pl.pallas_call(
        weave_kernel,
        grid=(slots, sources),
        in_specs=[spec, spec],
        out_specs=pl.BlockSpec(
            (1, 1, tokens, 2, width), lambda slot, source: (0, slot, source, 0, 0)
        ),
        out_shape=jax.ShapeDtypeStruct((1, slots, sources * tokens, 2, width), jnp.bfloat16),
        cost_estimate=pl.CostEstimate(
            flops=1024 * slots * sources * tokens * width,
            bytes_accessed=8 * slots * sources * tokens * width,
            transcendentals=0,
        ),
    )(keys, values)


def slot_hits(owners, decoders):
    requests = owners.shape[0]
    order = jnp.arange(requests, dtype=jnp.int32)
    same = owners[:, None] == owners[None, :]
    slot_of = jnp.sum((same & (order[None, :] < order[:, None])).astype(jnp.int32), axis=1)
    slot_hit = slot_of[None, :] == jnp.arange(CAP, dtype=jnp.int32)[:, None]
    owner_hit = owners[None, :] == jnp.arange(decoders, dtype=jnp.int32)[:, None]
    return owner_hit[:, None, :] & slot_hit[None, :, :]


def hand_over(arrived, hits, after):
    if after is not None:
        arrived = lax.optimization_barrier((arrived, after))[0]
    outgoing = jnp.zeros(hits.shape[:2] + arrived.shape[1:], arrived.dtype)
    for request in range(arrived.shape[0]):
        outgoing = jnp.where(
            hits[:, :, request][:, :, None, None], arrived[request][None, None], outgoing
        )
    landed = lax.all_to_all(outgoing, "seq", split_axis=0, concat_axis=0, tiled=True)
    return landed, outgoing


def body(
    prompt,
    key_value_weight,
    adapter_down_weight,
    adapter_up_weight,
    request_adapter_index,
    destination,
    rotated_query,
    key_value_cache,
    current_key_value,
    cached_length,
    row_adapter_index,
    output_weight,
    output_down_weight,
    output_up_weight,
):
    requests, tok_dev, model_width = prompt.shape
    width = key_value_weight.shape[2]
    shard = key_value_weight.shape[0]
    decoders = lax.axis_size("seq")
    heads = lax.axis_size("head")
    columns = 2 * ADAPTER_RANK
    tokens = prompt.reshape(requests * tok_dev, model_width)

    share = requests // heads if requests % heads == 0 else requests
    mine = lax.axis_index("head") * share if share < requests else 0
    my_adapter = lax.dynamic_slice_in_dim(request_adapter_index, mine, share)
    column = jnp.arange(ADAPTER_COUNT * columns, dtype=jnp.int32)
    wanted = my_adapter[:, None] * columns + jnp.arange(columns, dtype=jnp.int32)[None, :]
    pick = (wanted.reshape(-1)[:, None] == column[None, :]).astype(jnp.bfloat16)
    down = lax.dot_general(
        pick, adapter_down_weight, (((1,), (1,)), ((), ())), preferred_element_type=jnp.float32
    ).astype(jnp.bfloat16)
    matrix = key_value_weight.reshape(shard, 2 * width)
    down_all, down_first = gathered(down, "seq")
    matrix = lax.optimization_barrier((matrix, down_first))[0]
    key_all, key_first = gathered(matrix[:, :width], "seq")
    value_all, _ = gathered(matrix[:, width:], "seq", key_all)
    key_all = key_all.reshape(model_width, width)
    value_all = value_all.reshape(model_width, width)
    rotated_query = lax.optimization_barrier((rotated_query, key_first))[0]

    attended = attend(rotated_query, key_value_cache, current_key_value, cached_length)
    attn_rows = gathered(attended, "seq")[0].reshape(-1, attended.shape[1])
    ranks = ADAPTER_COUNT * ADAPTER_RANK
    down_flat = output_down_weight.reshape(output_down_weight.shape[0], ranks)
    up_flat = output_up_weight.reshape(ranks, output_up_weight.shape[2])
    rank_owner = jnp.arange(ranks, dtype=jnp.int32) // ADAPTER_RANK
    low_rows = jnp.dot(attn_rows, down_flat, preferred_element_type=jnp.float32)
    low_rows = jnp.where(row_adapter_index[:, None] == rank_owner[None, :], low_rows, 0.0)
    terms = jnp.dot(attn_rows, output_weight, preferred_element_type=jnp.float32)
    terms = terms + jnp.dot(
        low_rows.astype(jnp.bfloat16), up_flat, preferred_element_type=jnp.float32
    )
    decoded = scattered_sum(terms, "head").astype(jnp.bfloat16)

    my_tokens = lax.dynamic_slice_in_dim(prompt, mine, share, axis=0)
    my_down = down_all.transpose(1, 0, 2).reshape(share, columns, model_width)
    my_low = jnp.einsum("rtk,rck->rct", my_tokens, my_down, preferred_element_type=jnp.float32)
    low = gathered(my_low, "head")[0] if share < requests else my_low[None]
    low = low.reshape(requests, 2, ADAPTER_RANK, tok_dev).astype(jnp.bfloat16)
    own = jnp.eye(requests, dtype=jnp.bool_)[None, :, None, :, None]
    spread = jnp.where(
        own, low.transpose(1, 0, 2, 3)[:, :, :, None, :], jnp.zeros((), jnp.bfloat16)
    ).reshape(2, requests * ADAPTER_RANK, requests * tok_dev)
    selector = request_adapter_index[:, None] == jnp.arange(ADAPTER_COUNT, dtype=jnp.int32)[None, :]
    up = jnp.einsum(
        "um,mdzt->duzt",
        selector.astype(jnp.bfloat16),
        adapter_up_weight,
        preferred_element_type=jnp.float32,
    ).astype(jnp.bfloat16)
    up = up.reshape(2, requests * ADAPTER_RANK, width)

    pool_index = lax.axis_index("pool")
    other_owners = lax.dynamic_slice_in_dim(destination, (1 - pool_index) * requests, requests)
    hits = slot_hits(other_owners, decoders)

    arrived = []
    for which, weight in enumerate((key_all, value_all)):
        base = jnp.dot(tokens, weight, preferred_element_type=jnp.float32)
        extra = lax.dot_general(
            spread[which], up[which], (((0,), (0,)), ((), ())), preferred_element_type=jnp.float32
        )
        block = (base + extra).astype(jnp.bfloat16).reshape(requests, tok_dev, width)
        arrived.append(exchanged(block, "pool", 1))
    handed, outgoing = [], block
    for blocks in arrived:
        landed, outgoing = hand_over(blocks, hits, outgoing)
        handed.append(landed)
    return (weave(handed[0], handed[1]), decoded)


MESH = pl.DeviceIdType.MESH
PIECES = 4
SLOTS = 3
TILE = 256
PART = 128


def serve_kernel(
    dest_ref,
    adapter_ref,
    length_ref,
    prompt_ref,
    wa_ref,
    wb_ref,
    down_ref,
    up_ref,
    query_ref,
    cache_ref,
    current_ref,
    keep_ref,
    ow_ref,
    odown_ref,
    oup_ref,
    out_ref,
    decoded_ref,
    w0,
    w1,
    pbuf,
    acc,
    cbuf,
    owbuf,
    qbuf,
    abuf,
    att_all,
    down_all,
    low_acc,
    low_all,
    terms,
    tsend,
    trecv,
    hsend,
    recvx0,
    recvx1,
    sibx0,
    sibx1,
    ysend,
    yrecv0,
    yrecv1,
    siby0,
    siby1,
    ssem,
    rsem,
    lsem,
):
    f32, bf16 = jnp.float32, jnp.bfloat16
    requests, tok, model = prompt_ref.shape
    shard = wa_ref.shape[0]
    half_width = 2 * shard
    heads = lax.axis_size("head")
    rows = query_ref.shape[0]
    q_heads = query_ref.shape[1] // HEAD_DIM
    columns = 2 * ADAPTER_RANK
    p, me, h = lax.axis_index("pool"), lax.axis_index("seq"), lax.axis_index("head")
    y, c = me // 2, me % 2
    sib, peer, far = y * 2 + 1 - c, (1 - y) * 2 + c, (1 - y) * 2 + 1 - c
    slots = requests - 1
    recvx, sibx = (recvx0, recvx1), (sibx0, sibx1)
    yrecv, siby = (yrecv0, yrecv1), (siby0, siby1)
    w = (w0, w1)

    names = {}

    def sem_of(name, index=0):
        if name not in names:
            raise KeyError(name)
        return names[name] + index

    at = 0
    for name, count in (
        ("ya", PIECES), ("xa", PIECES), ("sa", 1), ("fa", 2), ("yb", 2), ("sb", 1), ("fb", 2),
        ("yd", 1), ("sd", 1), ("fd", 1), ("yt", 1), ("st", 1), ("ft", 1),
        ("zl", heads - 1), ("zt", heads - 1),
        ("hx", 2 * requests), ("hs", 2 * requests), ("hy", 2 * slots), ("hf", 2 * slots),
    ):
        names[name] = at
        at += count

    sent = []

    def remote(src, dst, name, index, target):
        i = sem_of(name, index)
        return pltpu.make_async_remote_copy(
            src_ref=src, dst_ref=dst, send_sem=ssem.at[i], recv_sem=rsem.at[i],
            device_id=target, device_id_type=MESH,
        )

    def send(src, dst, name, index, target, keep=True):
        copy = remote(src, dst, name, index, target)
        copy.start()
        if keep:
            sent.append(copy)

    def arrive(dst, name, index, target):
        remote(dst, dst, name, index, target).wait_recv()

    to_sib, to_peer, to_x = {"seq": sib}, {"seq": peer}, {"pool": 1 - p}

    def rows_of(ref, start, size):
        return ref.at[pl.ds(pl.multiple_of(start, PART), size)]

    barrier = pltpu.get_barrier_semaphore()
    partners = [to_sib, to_peer, to_x] + [{"head": (h + k) % heads} for k in range(1, heads)]
    for partner in partners:
        pl.semaphore_signal(barrier, inc=1, device_id=partner, device_id_type=MESH)
    pl.semaphore_wait(barrier, len(partners))

    piece = shard // (2 * PIECES)

    def y_piece(k):
        row = (p * PIECES + k) * piece
        send(rows_of(wa_ref, row, piece), rows_of(w0, me * shard + row, piece), "ya", k, to_peer)

    def y_arrived(k):
        row = peer * shard + (p * PIECES + k) * piece
        arrive(rows_of(w0, row, piece), "ya", k, to_peer)
        send(rows_of(w0, row, piece), rows_of(w0, row, piece), "xa", k, to_x)

    def x_arrived(k):
        row = peer * shard + ((1 - p) * PIECES + k) * piece
        arrive(rows_of(w0, row, piece), "xa", k, to_x)

    def prompt_load(step):
        if isinstance(step, int) and step < 2:
            r, half = h, (y if step == 0 else 1 - y)
        else:
            t = step - 2
            r, turn = t % requests, (t // requests) % 2
            half = turn + y - 2 * turn * y
        slot = step % SLOTS
        return pltpu.make_async_copy(
            prompt_ref.at[r, :, pl.ds(pl.multiple_of(half * half_width, half_width), half_width)],
            pbuf.at[slot],
            lsem.at[slot],
        )

    total_steps = 2 + 4 * requests
    y_piece(0)
    y_piece(1)
    cache_copy = pltpu.make_async_copy(cache_ref, cbuf, lsem.at[SLOTS])
    cache_copy.start()
    own_a = pltpu.make_async_copy(wa_ref, rows_of(w0, me * shard, shard), lsem.at[SLOTS + 1])
    own_b = pltpu.make_async_copy(wb_ref, rows_of(w1, me * shard, shard), lsem.at[SLOTS + 2])
    own_a.start()
    send(wa_ref, rows_of(w0, me * shard, shard), "sa", 0, to_sib)

    pick_row = lax.broadcasted_iota(jnp.int32, (columns, down_ref.shape[1]), 0)
    pick_col = lax.broadcasted_iota(jnp.int32, (columns, down_ref.shape[1]), 1)
    pick = jnp.where(pick_col == pick_row + adapter_ref[h] * columns, 1.0, 0.0).astype(bf16)
    my_cols = pl.ds(pl.multiple_of(me * shard, shard), shard)
    down_all[:, my_cols] = lax.dot_general(
        pick, down_ref[...], (((1,), (1,)), ((), ())), preferred_element_type=f32
    ).astype(bf16)
    for step in range(SLOTS):
        prompt_load(step).start()
    own_b.start()

    def ow_load(n):
        width = owbuf.shape[2]
        return pltpu.make_async_copy(
            ow_ref.at[:, pl.ds(pl.multiple_of(n * width, width), width)],
            owbuf.at[n % 2],
            lsem.at[SLOTS + 3 + n % 2],
        )

    for head in range(q_heads):
        qbuf[pl.ds(head, rows, stride=q_heads), :] = query_ref[
            :, head * HEAD_DIM : (head + 1) * HEAD_DIM
        ].astype(f32)
    down_view = down_all.at[:, my_cols]
    send(down_view, down_view, "yd", 0, to_peer)
    send(down_view, down_view, "sd", 0, to_sib)
    y_piece(2)
    y_piece(3)
    send(wb_ref, rows_of(w1, me * shard, shard), "sb", 0, to_sib)
    ow_load(0).start()
    ow_load(1).start()
    cache_copy.wait()

    positions = cache_ref.shape[1]
    kv_heads = current_ref.shape[2] // HEAD_DIM
    groups = q_heads // kv_heads
    batch = 8
    factor = HEAD_DIM ** (-0.5)
    lane = lax.broadcasted_iota(jnp.int32, (groups, 2 * positions), 1)

    def attend_step(step):
        start = step * batch
        blocks, scores, owns, values = [], [], [], []
        for row in range(batch):
            pairs = cbuf[start + row].reshape(2 * positions, kv_heads * HEAD_DIM)
            valid = (lane % 2 == 0) & (lane < 2 * length_ref[start + row])
            now = current_ref[start + row].astype(f32)
            for head in range(kv_heads):
                span = slice(head * HEAD_DIM, (head + 1) * HEAD_DIM)
                block = pairs[:, span]
                query = qbuf[
                    pl.ds(pl.multiple_of((start + row) * q_heads + head * groups, groups), groups), :
                ]
                own = jnp.sum(query * now[0:1, span], axis=1, keepdims=True) * factor
                score = lax.dot_general(
                    query.astype(bf16), block, (((1,), (1,)), ((), ())), preferred_element_type=f32
                )
                blocks.append(block)
                scores.append(jnp.where(valid, score * factor, -1e30))
                owns.append(own)
                values.append(now[1:2, span])
        score = jnp.concatenate(scores, axis=0)
        own = jnp.concatenate(owns, axis=0)
        highest = jnp.maximum(jnp.max(score, axis=1, keepdims=True), own)
        raw = jnp.where(score > -1e29, jnp.exp(score - highest), 0.0)
        own_raw = jnp.exp(own - highest)
        normer = jnp.sum(raw, axis=1, keepdims=True) + own_raw
        weights = pltpu.roll(raw / normer, 1, 1).astype(bf16)
        own_weight = (own_raw / normer).astype(bf16).astype(f32)
        for item in range(batch * kv_heads):
            at_row = item * groups
            mixed = jnp.dot(
                weights[at_row : at_row + groups], blocks[item], preferred_element_type=f32
            )
            abuf[
                pl.ds(pl.multiple_of(start * q_heads + at_row, groups), groups), :
            ] = mixed + own_weight[at_row : at_row + groups] * values[item]

    batches = rows // batch
    per = -(-batches // (PIECES - 1))
    for k in range(PIECES - 1):
        first, last = k * per, min(batches, (k + 1) * per)
        if first < last:
            pl.loop(first, last)(attend_step)
        y_arrived(k)

    for head in range(q_heads):
        att_all[me, :, head * HEAD_DIM : (head + 1) * HEAD_DIM] = abuf[
            pl.ds(head, rows, stride=q_heads), :
        ].astype(bf16)
    send(att_all.at[me], att_all.at[me], "yt", 0, to_peer)
    send(att_all.at[me], att_all.at[me], "st", 0, to_sib)
    half_shard = shard // 2
    for k in range(2):
        send(
            rows_of(wb_ref, k * half_shard, half_shard),
            rows_of(w1, me * shard + k * half_shard, half_shard), "yb", k, to_peer,
        )
    y_arrived(PIECES - 1)
    peer_part = rows_of(w0, peer * shard + p * half_shard, half_shard)
    send(peer_part, peer_part, "fa", 0, to_sib)

    def cols_at(who):
        return down_all.at[:, pl.ds(pl.multiple_of(who * shard, shard), shard)]

    arrive(cols_at(peer), "yd", 0, to_peer)
    send(cols_at(peer), cols_at(peer), "fd", 0, to_sib)
    arrive(cols_at(sib), "sd", 0, to_sib)
    arrive(cols_at(far), "fd", 0, to_sib)

    tiles = tok // TILE
    for step in range(2):
        prompt_load(step).wait()
        half = y if step == 0 else 1 - y
        cols = pl.ds(pl.multiple_of(half * half_width, half_width), half_width)

        @pl.loop(0, tiles)
        def _(i):
            at_row = pl.ds(pl.multiple_of(i * TILE, TILE), TILE)
            part = lax.dot_general(
                pbuf[step, at_row, :], down_all[:, cols], (((1,), (1,)), ((), ())),
                preferred_element_type=f32,
            )
            if step == 0:
                low_acc[at_row, :] = part
            else:
                low = jnp.concatenate(
                    [low_acc[at_row, :] + part, jnp.zeros((TILE, PART - columns), f32)], axis=1
                )
                low_all[h, at_row, :] = low.astype(bf16)

        prompt_load(step + SLOTS).start()
    for k in range(1, heads):
        send(low_all.at[h], low_all.at[h], "zl", k - 1, {"head": (h + k) % heads})

    def base_loop(ch, first, ready):
        @pl.loop(0, requests)
        def _(r):
            step = first + r
            prompt_load(step).wait()

            @pl.loop(0, tiles)
            def _(i):
                at_row = pl.ds(pl.multiple_of(i * TILE, TILE), TILE)
                weight = w[ch][pl.ds(pl.multiple_of(y * half_width, half_width), half_width), :]
                acc[r, at_row, :] = jnp.dot(
                    pbuf[step % SLOTS, at_row, :], weight, preferred_element_type=f32
                )

            prompt_load(step + SLOTS).start()

    order_row = lax.broadcasted_iota(jnp.int32, (2 * PART, 2 * PART), 0)
    order_col = lax.broadcasted_iota(jnp.int32, (2 * PART, 2 * PART), 1)
    order = jnp.where(order_col == (order_row % 2) * PART + order_row // 2, 1.0, 0.0).astype(bf16)

    def final_loop(ch, first):
        lanes = slice(ch * PART, (ch + 1) * PART)

        @pl.loop(0, requests)
        def _(r):
            step = first + r
            prompt_load(step).wait()
            adapter = adapter_ref[r]
            up_key, up_value = up_ref[adapter, 0][:, lanes], up_ref[adapter, 1][:, lanes]
            gap = jnp.zeros_like(up_key)
            up = jnp.concatenate(
                [
                    jnp.concatenate([up_key, gap], axis=1),
                    jnp.concatenate([gap, up_value], axis=1),
                    jnp.zeros((PART - columns, 2 * PART), bf16),
                ],
                axis=0,
            )

            @pl.loop(0, tiles)
            def _(i):
                at_row = pl.ds(pl.multiple_of(i * TILE, TILE), TILE)
                weight = w[ch][
                    pl.ds(pl.multiple_of((1 - y) * half_width, half_width), half_width), :
                ]
                value = (
                    acc[r, at_row, :]
                    + jnp.dot(
                        pbuf[step % SLOTS, at_row, :], weight, preferred_element_type=f32
                    )
                    + jnp.dot(low_all[r, at_row, :], up, preferred_element_type=f32)
                ).astype(bf16)
                for sub in range(TILE // PART):
                    x = value[sub * PART : (sub + 1) * PART]
                    both = jnp.concatenate([x[:, :PART], x[:, PART:]], axis=0)
                    woven = jnp.dot(order, both, preferred_element_type=f32).astype(bf16)
                    hsend[
                        ch, r,
                        pl.ds(pl.multiple_of(2 * (i * TILE + sub * PART), 2 * PART), 2 * PART), :,
                    ] = woven

            remote(
                hsend.at[ch, r], recvx[ch].at[r], "hx", ch * requests + r, to_x
            ).start()

            @pl.when(step + SLOTS < total_steps)
            def _():
                prompt_load(step + SLOTS).start()

    own_a.wait()
    arrive(rows_of(w0, sib * shard, shard), "sa", 0, to_sib)
    base_loop(0, 2, None)
    for k in range(PIECES):
        x_arrived(k)
    peer_other = rows_of(w0, peer * shard + (1 - p) * half_shard, half_shard)
    send(peer_other, peer_other, "fa", 1, to_sib)
    for k in range(1, heads):
        source = (h + heads - k) % heads
        arrive(low_all.at[source], "zl", k - 1, {"head": source})
    for k in range(2):
        pool_part = p + k - 2 * k * p
        arrive(rows_of(w0, far * shard + pool_part * half_shard, half_shard), "fa", k, to_sib)
    final_loop(0, 2 + requests)

    arrive(att_all.at[peer], "yt", 0, to_peer)
    send(att_all.at[peer], att_all.at[peer], "ft", 0, to_sib)
    arrive(att_all.at[sib], "st", 0, to_sib)
    arrive(att_all.at[far], "ft", 0, to_sib)
    members = att_all.shape[0]
    attended = att_all[...].reshape(members * rows, q_heads * HEAD_DIM)
    low_rows = lax.dot_general(
        attended, odown_ref[...], (((1,), (1,)), ((), ())), preferred_element_type=f32
    )
    low_rows = jnp.where(keep_ref[...] > 0.5, low_rows, 0.0).astype(bf16)
    ow_width = owbuf.shape[2]
    blocks = ow_ref.shape[1] // ow_width

    @pl.loop(0, blocks)
    def _(n):
        ow_load(n).wait()
        cols = pl.ds(pl.multiple_of(n * ow_width, ow_width), ow_width)
        part = jnp.dot(
            att_all[...].reshape(members * rows, q_heads * HEAD_DIM), owbuf[n % 2],
            preferred_element_type=f32,
        ) + jnp.dot(low_rows, oup_ref[:, cols], preferred_element_type=f32)
        terms[:, :, cols] = part.reshape(heads, rows, ow_width)

        @pl.when(n + 2 < blocks)
        def _():
            ow_load(n + 2).start()

    for k in range(1, heads):
        target = (h + k) % heads
        tsend[k - 1] = terms[target].astype(bf16)
        send(tsend.at[k - 1], trecv.at[k - 1], "zt", k - 1, {"head": target})

    arrive(rows_of(w1, sib * shard, shard), "sb", 0, to_sib)
    own_b.wait()
    base_loop(1, 2 + 2 * requests, None)

    base = (1 - p) * requests
    owner = [dest_ref[base + r] for r in range(requests)]
    away = [jnp.where(owner[r] // 2 == y, 0, 1) for r in range(requests)]

    def passed_home(j):
        kept = 1 - away[0]
        for r in range(1, j + 1):
            kept = jnp.maximum(kept, 1 - away[r])
        return kept

    def passed_away(j):
        kept = away[0]
        for r in range(1, j + 1):
            kept = jnp.maximum(kept, away[r])
        return kept

    chosen = []
    for s in range(CAP):
        index, found = 0, 0
        for r in range(requests):
            before = sum([jnp.where(owner[q] == owner[r], 1, 0) for q in range(r)], 0)
            hit = jnp.where((owner[r] == me) & (before == s), 1, 0)
            shift = passed_away(r - 1) if r > 0 else 0
            index = index + hit * r
            found = found + hit
            chosen_slot = hit * (r - shift)
            if r == 0:
                slot = chosen_slot
            else:
                slot = slot + chosen_slot
        chosen.append((found, index, jnp.clip(slot, 0, slots - 1)))

    def on_x(ch, r):
        arrive(recvx[ch].at[r], "hx", ch * requests + r, to_x)
        send(recvx[ch].at[r], sibx[ch].at[r], "hs", ch * requests + r, to_sib)
        if r >= 1:
            j = r - 1
            late = jnp.full((1, 1), passed_home(j), jnp.int32) > 0
            ysend[ch * slots + j] = jnp.where(late, recvx[ch][r], recvx[ch][j])
            send(ysend.at[ch * slots + j], yrecv[ch].at[j], "hy", ch * slots + j, to_peer)

    def on_y(ch, j):
        arrive(yrecv[ch].at[j], "hy", ch * slots + j, to_peer)
        send(yrecv[ch].at[j], siby[ch].at[j], "hf", ch * slots + j, to_sib)

    def place(ch, source, ref, by_slot):
        for s, (found, index, slot) in enumerate(chosen):
            got = jnp.full((1, 1), found, jnp.int32) > 0
            value = ref[slot if by_slot else index]
            out_ref[s, source, ch] = jnp.where(got, value, jnp.zeros_like(value))

    def place_x(ch):
        for r in range(requests):
            arrive(sibx[ch].at[r], "hs", ch * requests + r, to_sib)
        place(ch, me, recvx[ch], False)
        place(ch, sib, sibx[ch], False)

    def place_y(ch):
        for j in range(slots):
            arrive(siby[ch].at[j], "hf", ch * slots + j, to_sib)
        place(ch, peer, yrecv[ch], True)
        place(ch, far, siby[ch], True)

    def wb_arrived(k):
        part = rows_of(w1, peer * shard + k * half_shard, half_shard)
        arrive(part, "yb", k, to_peer)
        send(part, part, "fb", k, to_sib)

    on_x(0, 0)
    wb_arrived(0)
    total = terms[h]
    for k in range(1, heads):
        arrive(trecv.at[k - 1], "zt", k - 1, {"head": (h + heads - k) % heads})
        total = total + trecv[k - 1].astype(f32)
    decoded_ref[...] = total.astype(bf16)
    for r in range(1, requests):
        on_x(0, r)
    wb_arrived(1)
    for k in range(2):
        arrive(rows_of(w1, far * shard + k * half_shard, half_shard), "fb", k, to_sib)
    final_loop(1, 2 + 3 * requests)
    on_y(0, 0)
    on_x(1, 0)
    on_y(0, 1)
    on_x(1, 1)
    for j in range(2, slots):
        on_y(0, j)
    place_x(0)
    place_y(0)
    for r in range(2, requests):
        on_x(1, r)
        on_y(1, r - 2)
    place_x(1)
    on_y(1, slots - 1)
    place_y(1)

    for ch in range(2):
        for r in range(requests):
            remote(
                hsend.at[ch, r], recvx[ch].at[r], "hx", ch * requests + r, to_x
            ).wait_send()
    for copy in sent:
        copy.wait_send()


def serve(
    prompt, key_value_weight, adapter_down_weight, adapter_up_weight, request_adapter_index,
    destination, rotated_query, key_value_cache, current_key_value, cached_length,
    row_adapter_index, output_weight, output_down_weight, output_up_weight,
):
    f32, bf16 = jnp.float32, jnp.bfloat16
    requests, tok, model = prompt.shape
    shard, _, width = key_value_weight.shape
    heads = lax.axis_size("head")
    members = lax.axis_size("seq")
    rows = rotated_query.shape[0]
    attn_width = rotated_query.shape[1]
    q_heads = attn_width // HEAD_DIM
    ranks = ADAPTER_COUNT * ADAPTER_RANK
    out_width = output_weight.shape[1]
    wa = key_value_weight[:, :, :PART].reshape(shard, 2 * PART)
    wb = key_value_weight[:, :, PART:].reshape(shard, 2 * PART)
    odown = output_down_weight.transpose(1, 2, 0).reshape(ranks, attn_width)
    oup = output_up_weight.reshape(ranks, out_width)
    rank_owner = jnp.arange(ranks, dtype=jnp.int32) // ADAPTER_RANK
    keep = (row_adapter_index[:, None] == rank_owner[None, :]).astype(f32)
    slots = requests - 1
    ow_width = out_width // 4
    block = (2 * tok, PART)
    sems = 64 + 8 * requests
    vmem, smem, hbm = (
        pl.BlockSpec(memory_space=pltpu.VMEM),
        pl.BlockSpec(memory_space=pltpu.SMEM),
        pl.BlockSpec(memory_space=pl.ANY),
    )
    out, decoded = pl.pallas_call(
        serve_kernel,
        in_specs=[smem, smem, smem, hbm, hbm, hbm, vmem, vmem, vmem, hbm, vmem, vmem, hbm, vmem, vmem],
        out_specs=[vmem, vmem],
        out_shape=[
            jax.ShapeDtypeStruct((CAP, members, 2) + block, bf16),
            jax.ShapeDtypeStruct((rows, out_width), bf16),
        ],
        scratch_shapes=[
            pltpu.VMEM((model, 2 * PART), bf16),
            pltpu.VMEM((model, 2 * PART), bf16),
            pltpu.VMEM((SLOTS, tok, 2 * shard), bf16),
            pltpu.VMEM((requests, tok, 2 * PART), f32),
            pltpu.VMEM(key_value_cache.shape, bf16),
            pltpu.VMEM((2, attn_width, ow_width), bf16),
            pltpu.VMEM((rows * q_heads, HEAD_DIM), f32),
            pltpu.VMEM((rows * q_heads, HEAD_DIM), f32),
            pltpu.VMEM((members, rows, attn_width), bf16),
            pltpu.VMEM((2 * ADAPTER_RANK, model), bf16),
            pltpu.VMEM((tok, 2 * ADAPTER_RANK), f32),
            pltpu.VMEM((requests, tok, PART), bf16),
            pltpu.VMEM((heads, rows, out_width), f32),
            pltpu.VMEM((heads - 1, rows, out_width), bf16),
            pltpu.VMEM((heads - 1, rows, out_width), bf16),
            pltpu.VMEM((2, requests) + block, bf16),
            pltpu.VMEM((requests,) + block, bf16),
            pltpu.VMEM((requests,) + block, bf16),
            pltpu.VMEM((requests,) + block, bf16),
            pltpu.VMEM((requests,) + block, bf16),
            pltpu.VMEM((2 * slots,) + block, bf16),
            pltpu.VMEM((slots,) + block, bf16),
            pltpu.VMEM((slots,) + block, bf16),
            pltpu.VMEM((slots,) + block, bf16),
            pltpu.VMEM((slots,) + block, bf16),
            pltpu.SemaphoreType.DMA((sems,)),
            pltpu.SemaphoreType.DMA((sems,)),
            pltpu.SemaphoreType.DMA((SLOTS + 5,)),
        ],
        compiler_params=pltpu.CompilerParams(
            collective_id=0, has_side_effects=True, vmem_limit_bytes=67043328
        ),
    )(
        destination, request_adapter_index, cached_length, prompt, wa, wb, adapter_down_weight,
        adapter_up_weight, rotated_query, key_value_cache, current_key_value, keep, output_weight,
        odown, oup,
    )
    handed = out.reshape(CAP, members, 2, tok, 2, PART).transpose(0, 1, 3, 4, 2, 5)
    return handed.reshape(1, CAP, members * tok, 2, width), decoded


def fits(mesh):
    return mesh.shape["seq"] == 4 and mesh.shape["pool"] == 2


def solution(mesh):
    in_specs = (
        P("pool", "seq", None),
        P("seq", None, "head"),
        P("seq", None),
        P(None, None, None, "head"),
        P("pool"),
        P(),
        P(("pool", "seq"), "head"),
        P(("pool", "seq"), None, None, "head"),
        P(("pool", "seq"), None, "head"),
        P(("pool", "seq")),
        P("pool"),
        P("head", "seq"),
        P("head", None, None),
        P(None, None, "seq"),
    )
    out_specs = (P(("pool", "seq"), None, None, None, "head"), P(("pool", "head"), "seq"))
    run = serve if fits(mesh) else body
    return jax.shard_map(run, mesh=mesh, in_specs=in_specs, out_specs=out_specs, check_vma=False)
```

```python
import jax
import jax.numpy as jnp
from jax import lax
from jax.experimental import pallas as pl
from jax.experimental.pallas import tpu as pltpu
from jax.sharding import PartitionSpec as P

HEAD_DIM = 128
ADAPTER_RANK = 16
ADAPTER_COUNT = 8
CAP = 2


def exchanged(value, axis, mask):
    pairs = [(source, source ^ mask) for source in range(lax.axis_size(axis))]
    return lax.ppermute(value, axis, pairs)


def gathered(value, axis, after=None):
    size = lax.axis_size(axis)
    index = lax.axis_index(axis)
    held = value[None]
    mask = size // 2
    arrived = None
    while mask >= 1:
        other = exchanged(held, axis, mask)
        if after is not None:
            other = lax.optimization_barrier((other, after))[0]
        arrived = other if arrived is None else arrived
        low_bit = (index // mask) % 2 == 0
        first = jnp.where(low_bit, held, other)
        second = jnp.where(low_bit, other, held)
        held = jnp.stack([first, second], axis=1).reshape((-1,) + value.shape)
        mask //= 2
    return held, arrived


def scattered_sum(value, axis):
    size = lax.axis_size(axis)
    index = lax.axis_index(axis)
    held = value.reshape((size, value.shape[0] // size) + value.shape[1:])
    mask = 1
    while mask < size:
        split = held.reshape((held.shape[0] // 2, 2) + held.shape[1:])
        low_bit = (index // mask) % 2 == 0
        keep = jnp.where(low_bit, split[:, 0], split[:, 1])
        give = jnp.where(low_bit, split[:, 1], split[:, 0])
        held = keep + exchanged(give, axis, mask)
        mask *= 2
    return held[0]


def attend_kernel(lengths, query_ref, cache_ref, key_ref, value_ref, out_ref):
    rows, positions = cache_ref.shape[0], cache_ref.shape[1]
    kv_heads = key_ref.shape[1]
    groups = query_ref.shape[1] // kv_heads
    start = pl.program_id(0) * rows
    lane = lax.broadcasted_iota(jnp.int32, (groups, 2 * positions), 1)
    factor = HEAD_DIM ** (-0.5)
    blocks, scores, owns = [], [], []
    for row in range(rows):
        pairs = cache_ref[row].reshape(2 * positions, kv_heads * HEAD_DIM)
        valid = (lane % 2 == 0) & (lane < 2 * lengths[start + row])
        for head in range(kv_heads):
            block = pairs[:, head * HEAD_DIM : (head + 1) * HEAD_DIM]
            query = query_ref[row, head * groups : (head + 1) * groups, :]
            own_key = key_ref[row, head : head + 1, :].astype(jnp.float32)
            own = jnp.sum(query.astype(jnp.float32) * own_key, axis=1, keepdims=True) * factor
            score = lax.dot_general(
                query, block, (((1,), (1,)), ((), ())), preferred_element_type=jnp.float32
            )
            blocks.append(block)
            scores.append(jnp.where(valid, score * factor, -1e30))
            owns.append(own)
    scores = jnp.concatenate(scores, axis=0)
    own = jnp.concatenate(owns, axis=0)
    highest = jnp.maximum(jnp.max(scores, axis=1, keepdims=True), own)
    raw = jnp.where(scores > -1e29, jnp.exp(scores - highest), 0.0)
    own_raw = jnp.exp(own - highest)
    total = jnp.sum(raw, axis=1, keepdims=True) + own_raw
    weights = pltpu.roll(raw / total, 1, 1).astype(jnp.bfloat16)
    own_weight = (own_raw / total).astype(jnp.bfloat16).astype(jnp.float32)
    for row in range(rows):
        for head in range(kv_heads):
            at = (row * kv_heads + head) * groups
            own_value = value_ref[row, head : head + 1, :].astype(jnp.float32)
            mixed = jnp.dot(
                weights[at : at + groups],
                blocks[row * kv_heads + head],
                preferred_element_type=jnp.float32,
            )
            out_ref[row, head * groups : (head + 1) * groups, :] = (
                mixed + own_weight[at : at + groups] * own_value
            ).astype(jnp.bfloat16)


def attend(query, cache, current, lengths):
    rows, positions, _, width = cache.shape
    kv_heads = width // HEAD_DIM
    heads = query.shape[1] // HEAD_DIM
    step = next(size for size in (8, 4, 2, 1) if rows % size == 0)
    query = query.reshape(rows, heads, HEAD_DIM)
    own_key = current[:, 0].reshape(rows, kv_heads, HEAD_DIM)
    own_value = current[:, 1].reshape(rows, kv_heads, HEAD_DIM)
    out = pl.pallas_call(
        attend_kernel,
        grid_spec=pltpu.PrefetchScalarGridSpec(
            num_scalar_prefetch=1,
            grid=(rows // step,),
            in_specs=[
                pl.BlockSpec((step, heads, HEAD_DIM), lambda i, _: (i, 0, 0)),
                pl.BlockSpec((step, positions, 2, width), lambda i, _: (i, 0, 0, 0)),
                pl.BlockSpec((step, kv_heads, HEAD_DIM), lambda i, _: (i, 0, 0)),
                pl.BlockSpec((step, kv_heads, HEAD_DIM), lambda i, _: (i, 0, 0)),
            ],
            out_specs=pl.BlockSpec((step, heads, HEAD_DIM), lambda i, _: (i, 0, 0)),
        ),
        out_shape=jax.ShapeDtypeStruct((rows, heads, HEAD_DIM), jnp.bfloat16),
        cost_estimate=pl.CostEstimate(
            flops=8 * rows * heads * positions * HEAD_DIM,
            bytes_accessed=4 * rows * positions * width,
            transcendentals=2 * rows * heads * positions,
        ),
    )(lengths, query, cache, own_key, own_value)
    return out.reshape(rows, heads * HEAD_DIM)


def weave_kernel(key_ref, value_ref, out_ref):
    tokens, width = key_ref.shape[2], key_ref.shape[3]
    part = 128
    row = lax.broadcasted_iota(jnp.int32, (2 * part, 2 * part), 0)
    column = lax.broadcasted_iota(jnp.int32, (2 * part, 2 * part), 1)
    order = jnp.where(column == (row % 2) * part + row // 2, 1.0, 0.0).astype(jnp.bfloat16)
    for at in range(0, tokens, part):
        both = jnp.concatenate(
            [key_ref[0, 0, at : at + part, :], value_ref[0, 0, at : at + part, :]], axis=0
        )
        woven = jnp.dot(order, both, preferred_element_type=jnp.float32).astype(jnp.bfloat16)
        out_ref[0, 0, at : at + part, :, :] = woven.reshape(part, 2, width)


def weave(keys, values):
    sources, slots, tokens, width = keys.shape
    spec = pl.BlockSpec((1, 1, tokens, width), lambda slot, source: (source, slot, 0, 0))
    return pl.pallas_call(
        weave_kernel,
        grid=(slots, sources),
        in_specs=[spec, spec],
        out_specs=pl.BlockSpec(
            (1, 1, tokens, 2, width), lambda slot, source: (0, slot, source, 0, 0)
        ),
        out_shape=jax.ShapeDtypeStruct((1, slots, sources * tokens, 2, width), jnp.bfloat16),
        cost_estimate=pl.CostEstimate(
            flops=1024 * slots * sources * tokens * width,
            bytes_accessed=8 * slots * sources * tokens * width,
            transcendentals=0,
        ),
    )(keys, values)


def slot_hits(owners, decoders):
    requests = owners.shape[0]
    order = jnp.arange(requests, dtype=jnp.int32)
    same = owners[:, None] == owners[None, :]
    slot_of = jnp.sum((same & (order[None, :] < order[:, None])).astype(jnp.int32), axis=1)
    slot_hit = slot_of[None, :] == jnp.arange(CAP, dtype=jnp.int32)[:, None]
    owner_hit = owners[None, :] == jnp.arange(decoders, dtype=jnp.int32)[:, None]
    return owner_hit[:, None, :] & slot_hit[None, :, :]


def hand_over(arrived, hits, after):
    if after is not None:
        arrived = lax.optimization_barrier((arrived, after))[0]
    outgoing = jnp.zeros(hits.shape[:2] + arrived.shape[1:], arrived.dtype)
    for request in range(arrived.shape[0]):
        outgoing = jnp.where(
            hits[:, :, request][:, :, None, None], arrived[request][None, None], outgoing
        )
    landed = lax.all_to_all(outgoing, "seq", split_axis=0, concat_axis=0, tiled=True)
    return landed, outgoing


def body(
    prompt,
    key_value_weight,
    adapter_down_weight,
    adapter_up_weight,
    request_adapter_index,
    destination,
    rotated_query,
    key_value_cache,
    current_key_value,
    cached_length,
    row_adapter_index,
    output_weight,
    output_down_weight,
    output_up_weight,
):
    requests, tok_dev, model_width = prompt.shape
    width = key_value_weight.shape[2]
    shard = key_value_weight.shape[0]
    decoders = lax.axis_size("seq")
    heads = lax.axis_size("head")
    columns = 2 * ADAPTER_RANK
    tokens = prompt.reshape(requests * tok_dev, model_width)

    share = requests // heads if requests % heads == 0 else requests
    mine = lax.axis_index("head") * share if share < requests else 0
    my_adapter = lax.dynamic_slice_in_dim(request_adapter_index, mine, share)
    column = jnp.arange(ADAPTER_COUNT * columns, dtype=jnp.int32)
    wanted = my_adapter[:, None] * columns + jnp.arange(columns, dtype=jnp.int32)[None, :]
    pick = (wanted.reshape(-1)[:, None] == column[None, :]).astype(jnp.bfloat16)
    down = lax.dot_general(
        pick, adapter_down_weight, (((1,), (1,)), ((), ())), preferred_element_type=jnp.float32
    ).astype(jnp.bfloat16)
    matrix = key_value_weight.reshape(shard, 2 * width)
    down_all, down_first = gathered(down, "seq")
    matrix = lax.optimization_barrier((matrix, down_first))[0]
    key_all, key_first = gathered(matrix[:, :width], "seq")
    value_all, _ = gathered(matrix[:, width:], "seq", key_all)
    key_all = key_all.reshape(model_width, width)
    value_all = value_all.reshape(model_width, width)
    rotated_query = lax.optimization_barrier((rotated_query, key_first))[0]

    attended = attend(rotated_query, key_value_cache, current_key_value, cached_length)
    attn_rows = gathered(attended, "seq")[0].reshape(-1, attended.shape[1])
    ranks = ADAPTER_COUNT * ADAPTER_RANK
    down_flat = output_down_weight.reshape(output_down_weight.shape[0], ranks)
    up_flat = output_up_weight.reshape(ranks, output_up_weight.shape[2])
    rank_owner = jnp.arange(ranks, dtype=jnp.int32) // ADAPTER_RANK
    low_rows = jnp.dot(attn_rows, down_flat, preferred_element_type=jnp.float32)
    low_rows = jnp.where(row_adapter_index[:, None] == rank_owner[None, :], low_rows, 0.0)
    terms = jnp.dot(attn_rows, output_weight, preferred_element_type=jnp.float32)
    terms = terms + jnp.dot(
        low_rows.astype(jnp.bfloat16), up_flat, preferred_element_type=jnp.float32
    )
    decoded = scattered_sum(terms, "head").astype(jnp.bfloat16)

    my_tokens = lax.dynamic_slice_in_dim(prompt, mine, share, axis=0)
    my_down = down_all.transpose(1, 0, 2).reshape(share, columns, model_width)
    my_low = jnp.einsum("rtk,rck->rct", my_tokens, my_down, preferred_element_type=jnp.float32)
    low = gathered(my_low, "head")[0] if share < requests else my_low[None]
    low = low.reshape(requests, 2, ADAPTER_RANK, tok_dev).astype(jnp.bfloat16)
    own = jnp.eye(requests, dtype=jnp.bool_)[None, :, None, :, None]
    spread = jnp.where(
        own, low.transpose(1, 0, 2, 3)[:, :, :, None, :], jnp.zeros((), jnp.bfloat16)
    ).reshape(2, requests * ADAPTER_RANK, requests * tok_dev)
    selector = request_adapter_index[:, None] == jnp.arange(ADAPTER_COUNT, dtype=jnp.int32)[None, :]
    up = jnp.einsum(
        "um,mdzt->duzt",
        selector.astype(jnp.bfloat16),
        adapter_up_weight,
        preferred_element_type=jnp.float32,
    ).astype(jnp.bfloat16)
    up = up.reshape(2, requests * ADAPTER_RANK, width)

    pool_index = lax.axis_index("pool")
    other_owners = lax.dynamic_slice_in_dim(destination, (1 - pool_index) * requests, requests)
    hits = slot_hits(other_owners, decoders)

    arrived = []
    for which, weight in enumerate((key_all, value_all)):
        base = jnp.dot(tokens, weight, preferred_element_type=jnp.float32)
        extra = lax.dot_general(
            spread[which], up[which], (((0,), (0,)), ((), ())), preferred_element_type=jnp.float32
        )
        block = (base + extra).astype(jnp.bfloat16).reshape(requests, tok_dev, width)
        arrived.append(exchanged(block, "pool", 1))
    handed, outgoing = [], block
    for blocks in arrived:
        landed, outgoing = hand_over(blocks, hits, outgoing)
        handed.append(landed)
    return (weave(handed[0], handed[1]), decoded)


MESH = pl.DeviceIdType.MESH
PIECES = 4
SLOTS = 3
SHARED = 1
OUTS = 8
TILE = 256
PART = 128


def serve_kernel(
    dest_ref,
    adapter_ref,
    length_ref,
    prompt_ref,
    kv_ref,
    down_hbm,
    up_hbm,
    query_hbm,
    cache_ref,
    current_hbm,
    row_ref,
    ow_ref,
    odown_hbm,
    oup_hbm,
    out_ref,
    decoded_ref,
    w0,
    w1,
    kraw,
    pbuf,
    acc,
    cbuf,
    owbuf,
    down_ref,
    up_ref,
    query_ref,
    current_ref,
    odown_ref,
    oup_ref,
    qbuf,
    abuf,
    att_all,
    down_all,
    low_acc,
    low_flat,
    low_all,
    terms,
    tsend,
    trecv,
    hsend,
    stage,
    recvx0,
    recvx1,
    sibx0,
    sibx1,
    ysend,
    yrecv0,
    yrecv1,
    siby0,
    siby1,
    ssem,
    rsem,
    lsem,
):
    f32, bf16 = jnp.float32, jnp.bfloat16
    requests, tok, model = prompt_ref.shape
    shard = kv_ref.shape[0]
    half_width = 2 * shard
    heads = lax.axis_size("head")
    rows = query_ref.shape[0]
    q_heads = query_ref.shape[1] // HEAD_DIM
    columns = 2 * ADAPTER_RANK
    p, me, h = lax.axis_index("pool"), lax.axis_index("seq"), lax.axis_index("head")
    y, c = me // 2, me % 2
    sib, peer, far = y * 2 + 1 - c, (1 - y) * 2 + c, (1 - y) * 2 + 1 - c
    slots = requests - 1
    tiles = tok // TILE
    recvx, sibx = (recvx0, recvx1), (sibx0, sibx1)
    yrecv, siby = (yrecv0, yrecv1), (siby0, siby1)
    w = (w0, w1)

    names, at = {}, 0
    for name, count in (
        ("ya", PIECES), ("xa", PIECES), ("sa", 1), ("fa", 2 * PIECES),
        ("yb", SHARED + 1), ("xb", SHARED), ("sb", 1), ("fb", 3),
        ("yd", 1), ("sd", 1), ("fd", 1), ("yt", 1), ("st", 1), ("ft", 1),
        ("zl", heads - 1), ("zt", heads - 1),
        ("hx", 2 * requests * tiles), ("hs", 2 * requests * tiles),
        ("hy", 2 * slots * tiles), ("hf", 2 * slots * tiles),
    ):
        names[name] = at
        at += count

    sent = []

    def remote(src, dst, name, index, target):
        i = names[name] + index
        return pltpu.make_async_remote_copy(
            src_ref=src, dst_ref=dst, send_sem=ssem.at[i], recv_sem=rsem.at[i],
            device_id=target, device_id_type=MESH,
        )

    def send(src, dst, name, index, target):
        copy = remote(src, dst, name, index, target)
        copy.start()
        sent.append(copy)

    def arrive(dst, name, index, target):
        remote(dst, dst, name, index, target).wait_recv()

    to_sib, to_peer, to_x = {"seq": sib}, {"seq": peer}, {"pool": 1 - p}

    def rows_of(ref, start, size):
        return ref.at[pl.ds(pl.multiple_of(start, PART), size)]

    def pass_on(part, name, index, target):
        send(part, part, name, index, target)

    def kv_load(ch):
        return pltpu.make_async_copy(
            kv_ref.at[:, :, ch * PART : (ch + 1) * PART], kraw.at[ch], lsem.at[SLOTS + 1 + ch]
        )

    ends = SLOTS + 5 + OUTS
    small = [
        pltpu.make_async_copy(src, dst, lsem.at[ends + i])
        for i, (src, dst) in enumerate(
            (
                (down_hbm, down_ref), (up_hbm, up_ref), (query_hbm, query_ref),
                (current_hbm, current_ref), (odown_hbm, odown_ref), (oup_hbm, oup_ref),
            )
        )
    ]

    def prompt_load(step):
        if isinstance(step, int) and step < requests:
            r, half = step, y
        elif isinstance(step, int) and step < requests + 2:
            r, half = h, (y if step == requests else 1 - y)
        else:
            t = step - 2
            r, turn = t % requests, (t // requests) % 2
            half = turn + y - 2 * turn * y
        slot = step % SLOTS
        return pltpu.make_async_copy(
            prompt_ref.at[r, :, pl.ds(pl.multiple_of(half * half_width, half_width), half_width)],
            pbuf.at[slot],
            lsem.at[slot],
        )

    def ow_load(n):
        width = owbuf.shape[2]
        return pltpu.make_async_copy(
            ow_ref.at[:, pl.ds(pl.multiple_of(n * width, width), width)],
            owbuf.at[n % 2],
            lsem.at[SLOTS + 3 + n % 2],
        )

    total_steps = 2 + 4 * requests
    kv_load(0).start()
    small[0].start()

    barrier = pltpu.get_barrier_semaphore()
    partners = [to_sib, to_peer, to_x] + [{"head": (h + k) % heads} for k in range(1, heads)]
    for partner in partners:
        pl.semaphore_signal(barrier, inc=1, device_id=partner, device_id_type=MESH)
    prompt_load(0).start()
    kv_load(1).start()
    for step in range(1, SLOTS):
        prompt_load(step).start()
    for copy in small[1:]:
        copy.start()
    cache_copy = pltpu.make_async_copy(cache_ref, cbuf, lsem.at[SLOTS])
    cache_copy.start()
    ow_load(0).start()
    ow_load(1).start()

    order_row = lax.broadcasted_iota(jnp.int32, (2 * PART, 2 * PART), 0)
    order_col = lax.broadcasted_iota(jnp.int32, (2 * PART, 2 * PART), 1)
    order = jnp.where(order_col == (order_row % 2) * PART + order_row // 2, 1.0, 0.0).astype(bf16)
    unorder = jnp.where(order_row == (order_col % 2) * PART + order_col // 2, 1.0, 0.0).astype(bf16)

    def split_rows(ch, start, size):
        @pl.loop(0, size // PART)
        def _(b):
            row = pl.multiple_of(start + b * PART, PART)
            pairs = kraw[ch, pl.ds(row, PART)].reshape(2 * PART, PART)
            parts = jnp.dot(unorder, pairs, preferred_element_type=f32).astype(bf16)
            to = pl.ds(pl.multiple_of(me * shard + row, PART), PART)
            w[ch][to, :PART] = parts[:PART]
            w[ch][to, PART:] = parts[PART:]

    piece = shard // (2 * PIECES)
    half_shard = shard // 2

    def y_piece(k):
        pass_on(rows_of(w0, me * shard + (p * PIECES + k) * piece, piece), "ya", k, to_peer)

    def y_arrived(k):
        part = rows_of(w0, peer * shard + (p * PIECES + k) * piece, piece)
        arrive(part, "ya", k, to_peer)
        pass_on(part, "xa", k, to_x)
        pass_on(part, "fa", k, to_sib)

    def x_arrived(k):
        part = rows_of(w0, peer * shard + ((1 - p) * PIECES + k) * piece, piece)
        arrive(part, "xa", k, to_x)
        pass_on(part, "fa", PIECES + k, to_sib)

    def far_arrived():
        for k in range(PIECES):
            for turn, pool_part in enumerate((p, 1 - p)):
                part = rows_of(w0, far * shard + (pool_part * PIECES + k) * piece, piece)
                arrive(part, "fa", turn * PIECES + k, to_sib)

    kv_load(0).wait()
    split_rows(0, p * half_shard, 2 * piece)
    pl.semaphore_wait(barrier, len(partners))
    y_piece(0)
    split_rows(0, p * half_shard + 2 * piece, 2 * piece)
    y_piece(1)

    small[0].wait()
    pick_row = lax.broadcasted_iota(jnp.int32, (columns, down_ref.shape[1]), 0)
    pick_col = lax.broadcasted_iota(jnp.int32, (columns, down_ref.shape[1]), 1)
    pick = jnp.where(pick_col == pick_row + adapter_ref[h] * columns, 1.0, 0.0).astype(bf16)

    def cols_at(who):
        return down_all.at[:, pl.ds(pl.multiple_of(who * shard, shard), shard)]

    down_all[:, pl.ds(pl.multiple_of(me * shard, shard), shard)] = lax.dot_general(
        pick, down_ref[...], (((1,), (1,)), ((), ())), preferred_element_type=f32
    ).astype(bf16)
    split_rows(0, (1 - p) * half_shard, half_shard)
    pass_on(cols_at(me), "yd", 0, to_peer)
    pass_on(cols_at(me), "sd", 0, to_sib)
    y_piece(2)
    y_piece(3)
    pass_on(rows_of(w0, me * shard, shard), "sa", 0, to_sib)

    def base(ch, r, step):
        prompt_load(step).wait()

        @pl.loop(0, tiles)
        def _(i):
            at_row = pl.ds(pl.multiple_of(i * TILE, TILE), TILE)
            weight = w[ch][pl.ds(pl.multiple_of(y * half_width, half_width), half_width), :]
            acc[r, at_row, :] = jnp.dot(
                pbuf[step % SLOTS, at_row, :], weight, preferred_element_type=f32
            )

        prompt_load(step + SLOTS).start()

    kv_load(1).wait()
    kept = shard - 2 * SHARED * piece
    mine_at = p * (shard - SHARED * piece)
    theirs_at = (1 - p) * (shard - SHARED * piece)
    split_rows(1, mine_at, SHARED * piece)
    for k in range(SHARED):
        pass_on(rows_of(w1, me * shard + mine_at + k * piece, piece), "yb", k, to_peer)
    split_rows(1, SHARED * piece, kept)
    pass_on(rows_of(w1, me * shard + SHARED * piece, kept), "yb", SHARED, to_peer)
    split_rows(1, theirs_at, SHARED * piece)

    arrive(rows_of(w0, sib * shard, shard), "sa", 0, to_sib)
    base(0, 0, 0)
    y_arrived(0)
    base(0, 1, 1)
    y_arrived(1)
    base(0, 2, 2)
    arrive(cols_at(peer), "yd", 0, to_peer)
    pass_on(cols_at(peer), "fd", 0, to_sib)
    for r in range(3, requests):
        base(0, r, r)
    y_arrived(2)

    pass_on(rows_of(w1, me * shard, shard), "sb", 0, to_sib)
    arrive(cols_at(sib), "sd", 0, to_sib)
    arrive(cols_at(far), "fd", 0, to_sib)

    for turn in range(2):
        step = requests + turn
        prompt_load(step).wait()
        half = y if turn == 0 else 1 - y
        cols = pl.ds(pl.multiple_of(half * half_width, half_width), half_width)

        @pl.loop(0, tiles)
        def _(i):
            at_row = pl.ds(pl.multiple_of(i * TILE, TILE), TILE)
            part = lax.dot_general(
                pbuf[step % SLOTS, at_row, :], down_all[:, cols], (((1,), (1,)), ((), ())),
                preferred_element_type=f32,
            )
            if turn == 0:
                low_acc[at_row, :] = part
            else:
                low = jnp.concatenate(
                    [low_acc[at_row, :] + part, jnp.zeros((TILE, PART - columns), f32)], axis=1
                )
                low_flat[h, i] = low.T[:columns].astype(bf16)

        prompt_load(step + SLOTS).start()
    for k in range(1, heads):
        pass_on(low_flat.at[h], "zl", k - 1, {"head": (h + k) % heads})
    y_arrived(3)
    for copy in small[1:]:
        copy.wait()

    def half_block(ref, index, i):
        return ref.at[index, pl.ds(pl.multiple_of(i * 2 * TILE, 2 * TILE), 2 * TILE)]

    def final(ch, r, step):
        lanes = slice(ch * PART, (ch + 1) * PART)
        prompt_load(step).wait()
        adapter = adapter_ref[r]
        up_key, up_value = up_ref[adapter, 0][:, lanes], up_ref[adapter, 1][:, lanes]
        gap = jnp.zeros_like(up_key)
        up = jnp.concatenate(
            [
                jnp.concatenate([up_key, gap], axis=1),
                jnp.concatenate([gap, up_value], axis=1),
                jnp.zeros((PART - columns, 2 * PART), bf16),
            ],
            axis=0,
        )

        @pl.loop(0, tiles)
        def _(i):
            at_row = pl.ds(pl.multiple_of(i * TILE, TILE), TILE)
            weight = w[ch][
                pl.ds(pl.multiple_of((1 - y) * half_width, half_width), half_width), :
            ]
            value = (
                acc[r, at_row, :]
                + jnp.dot(pbuf[step % SLOTS, at_row, :], weight, preferred_element_type=f32)
                + jnp.dot(low_all[r, at_row, :], up, preferred_element_type=f32)
            ).astype(bf16)
            for sub in range(TILE // PART):
                x = value[sub * PART : (sub + 1) * PART]
                both = jnp.concatenate([x[:, :PART], x[:, PART:]], axis=0)
                woven = jnp.dot(order, both, preferred_element_type=f32).astype(bf16)
                hsend[
                    ch * requests + r,
                    pl.ds(pl.multiple_of(2 * (i * TILE + sub * PART), 2 * PART), 2 * PART), :,
                ] = woven
            remote(
                half_block(hsend, ch * requests + r, i), half_block(recvx[ch], r, i),
                "hx", (ch * requests + r) * tiles + i, to_x,
            ).start()

        if step + SLOTS < total_steps:
            prompt_load(step + SLOTS).start()

    for head in range(q_heads):
        qbuf[pl.ds(head, rows, stride=q_heads), :] = query_ref[
            :, head * HEAD_DIM : (head + 1) * HEAD_DIM
        ].astype(f32)
    cache_copy.wait()
    positions = cache_ref.shape[1]
    kv_heads = current_ref.shape[2] // HEAD_DIM
    groups = q_heads // kv_heads
    batch = 8
    factor = HEAD_DIM ** (-0.5)
    lane = lax.broadcasted_iota(jnp.int32, (groups, 2 * positions), 1)

    batches = rows // batch

    def attend_step(step):
        start = step * batch
        blocks, scores, owns, values = [], [], [], []
        for row in range(batch):
            pairs = cbuf[start + row].reshape(2 * positions, kv_heads * HEAD_DIM)
            valid = (lane % 2 == 0) & (lane < 2 * length_ref[start + row])
            now = current_ref[start + row].astype(f32)
            for head in range(kv_heads):
                span = slice(head * HEAD_DIM, (head + 1) * HEAD_DIM)
                block = pairs[:, span]
                query = qbuf[
                    pl.ds(pl.multiple_of((start + row) * q_heads + head * groups, groups), groups), :
                ]
                own = jnp.sum(query * now[0:1, span], axis=1, keepdims=True) * factor
                score = lax.dot_general(
                    query.astype(bf16), block, (((1,), (1,)), ((), ())), preferred_element_type=f32
                )
                blocks.append(block)
                scores.append(jnp.where(valid, score * factor, -1e30))
                owns.append(own)
                values.append(now[1:2, span])
        score = jnp.concatenate(scores, axis=0)
        own = jnp.concatenate(owns, axis=0)
        highest = jnp.maximum(jnp.max(score, axis=1, keepdims=True), own)
        raw = jnp.where(score > -1e29, jnp.exp(score - highest), 0.0)
        own_raw = jnp.exp(own - highest)
        normer = jnp.sum(raw, axis=1, keepdims=True) + own_raw
        weights = pltpu.roll(raw / normer, 1, 1).astype(bf16)
        own_weight = (own_raw / normer).astype(bf16).astype(f32)
        for item in range(batch * kv_heads):
            at_row = item * groups
            mixed = jnp.dot(
                weights[at_row : at_row + groups], blocks[item], preferred_element_type=f32
            )
            abuf[
                pl.ds(pl.multiple_of(start * q_heads + at_row, groups), groups), :
            ] = mixed + own_weight[at_row : at_row + groups] * values[item]

    def attend(start, stop):
        pl.loop(start, stop)(attend_step)

    attend(0, batches // 3)
    for k in range(PIECES - 1):
        x_arrived(k)
    attend(batches // 3, batches - batches // 3)
    x_arrived(PIECES - 1)
    for k in range(1, heads):
        source = (h + heads - k) % heads
        arrive(low_flat.at[source], "zl", k - 1, {"head": source})

    @pl.loop(0, requests)
    def _(r):
        for i in range(tiles):
            low = jnp.concatenate(
                [low_flat[r, i].astype(f32), jnp.zeros((PART - columns, TILE), f32)], axis=0
            )
            low_all[r, i * TILE : (i + 1) * TILE, :] = low.T.astype(bf16)

    far_arrived()

    def shared_arrived(k):
        part = rows_of(w1, peer * shard + mine_at + k * piece, piece)
        arrive(part, "yb", k, to_peer)
        pass_on(part, "xb", k, to_x)

    first = 2 + requests
    for r in range(requests):
        final(0, r, first + r)
        if r < SHARED:
            shared_arrived(r)
    pass_on(rows_of(w1, peer * shard + mine_at, SHARED * piece), "fb", 0, to_sib)

    attend(batches - batches // 3, batches)
    for head in range(q_heads):
        att_all[me, :, head * HEAD_DIM : (head + 1) * HEAD_DIM] = abuf[
            pl.ds(head, rows, stride=q_heads), :
        ].astype(bf16)
    pass_on(att_all.at[me], "yt", 0, to_peer)
    pass_on(att_all.at[me], "st", 0, to_sib)

    other = (1 - p) * requests
    owner = [dest_ref[other + r] for r in range(requests)]
    away = [jnp.where(owner[r] // 2 == y, 0, 1) for r in range(requests)]

    def some(flags):
        kept = flags[0]
        for flag in flags[1:]:
            kept = jnp.maximum(kept, flag)
        return kept

    chosen = []
    for s in range(CAP):
        index, found, slot = 0, 0, 0
        for r in range(requests):
            before = sum([jnp.where(owner[q] == owner[r], 1, 0) for q in range(r)], 0)
            hit = jnp.where((owner[r] == me) & (before == s), 1, 0)
            shift = some(away[:r]) if r > 0 else 0
            index, found, slot = index + hit * r, found + hit, slot + hit * (r - shift)
        chosen.append((found, index, jnp.clip(slot, 0, slots - 1)))

    def on_x(ch, r, i):
        part = half_block(recvx[ch], r, i)
        arrive(part, "hx", (ch * requests + r) * tiles + i, to_x)
        send(part, half_block(sibx[ch], r, i), "hs", (ch * requests + r) * tiles + i, to_sib)
        if r >= 1:
            j = r - 1
            span = slice(i * 2 * TILE, (i + 1) * 2 * TILE)
            late = jnp.full((1, 1), some([1 - a for a in away[: j + 1]]), jnp.int32) > 0
            ysend[ch * slots + j, span] = jnp.where(late, recvx[ch][r, span], recvx[ch][j, span])
            send(
                half_block(ysend, ch * slots + j, i), half_block(yrecv[ch], j, i),
                "hy", (ch * slots + j) * tiles + i, to_peer,
            )

    def on_y(ch, j, i):
        part = half_block(yrecv[ch], j, i)
        arrive(part, "hy", (ch * slots + j) * tiles + i, to_peer)
        send(part, half_block(siby[ch], j, i), "hf", (ch * slots + j) * tiles + i, to_sib)

    placed = []

    def place(ch, source, ref, by_slot, i):
        span = pl.ds(i * 2 * TILE, 2 * TILE)
        for s, (found, index, slot) in enumerate(chosen):
            got = jnp.full((1, 1), found, jnp.int32) > 0
            value = ref[slot if by_slot else index, span]
            turn = len(placed)
            if turn >= OUTS:
                placed[turn - OUTS].wait()
            stage[turn % OUTS] = jnp.where(got, value, jnp.zeros_like(value))
            copy = pltpu.make_async_copy(
                stage.at[turn % OUTS], out_ref.at[s, source, ch, span],
                lsem.at[SLOTS + 5 + turn % OUTS],
            )
            copy.start()
            placed.append(copy)

    def place_x(ch):
        for i in range(tiles):
            place(ch, me, recvx[ch], False, i)
        for r in range(requests):
            for i in range(tiles):
                arrive(half_block(sibx[ch], r, i), "hs", (ch * requests + r) * tiles + i, to_sib)
        for i in range(tiles):
            place(ch, sib, sibx[ch], False, i)

    def place_y(ch):
        for i in range(tiles):
            place(ch, peer, yrecv[ch], True, i)
        for j in range(slots):
            for i in range(tiles):
                arrive(half_block(siby[ch], j, i), "hf", (ch * slots + j) * tiles + i, to_sib)
        for i in range(tiles):
            place(ch, far, siby[ch], True, i)

    x_queue = [(ch, r, i) for ch in range(2) for r in range(requests) for i in range(tiles)]
    y_queue = [(ch, j, i) for ch in range(2) for j in range(slots) for i in range(tiles)]

    def take_x(count):
        for _ in range(count):
            on_x(*x_queue.pop(0))

    def take_y(count):
        for _ in range(count):
            on_y(*y_queue.pop(0))

    def project():
        arrive(att_all.at[sib], "st", 0, to_sib)
        arrive(att_all.at[far], "ft", 0, to_sib)
        members = att_all.shape[0]
        low_rows = lax.dot_general(
            odown_ref[...], att_all[...].reshape(members * rows, q_heads * HEAD_DIM),
            (((1,), (1,)), ((), ())), preferred_element_type=f32,
        )
        rank_owner = lax.broadcasted_iota(jnp.int32, low_rows.shape, 0) // ADAPTER_RANK
        low_rows = jnp.where(rank_owner == row_ref[...], low_rows, 0.0).astype(bf16)
        ow_width = owbuf.shape[2]
        blocks = ow_ref.shape[1] // ow_width

        @pl.loop(0, blocks)
        def _(n):
            ow_load(n).wait()
            cols = pl.ds(pl.multiple_of(n * ow_width, ow_width), ow_width)
            part = jnp.dot(
                att_all[...].reshape(members * rows, q_heads * HEAD_DIM), owbuf[n % 2],
                preferred_element_type=f32,
            ) + lax.dot_general(
                low_rows, oup_ref[:, cols], (((0,), (0,)), ((), ())), preferred_element_type=f32
            )
            terms[:, :, cols] = part.reshape(heads, rows, ow_width)

            @pl.when(n + 2 < blocks)
            def _():
                ow_load(n + 2).start()

        for k in range(1, heads):
            target = (h + k) % heads
            tsend[k - 1] = terms[target].astype(bf16)
            send(tsend.at[k - 1], trecv.at[k - 1], "zt", k - 1, {"head": target})

    take_x(tiles)
    arrive(rows_of(w1, sib * shard, shard), "sb", 0, to_sib)
    first = 2 + 2 * requests
    for r in range(requests):
        base(1, r, first + r)
    part = rows_of(w1, peer * shard + SHARED * piece, kept)
    arrive(part, "yb", SHARED, to_peer)
    pass_on(part, "fb", 1, to_sib)
    for k in range(SHARED):
        arrive(rows_of(w1, peer * shard + theirs_at + k * piece, piece), "xb", k, to_x)
    pass_on(rows_of(w1, peer * shard + theirs_at, SHARED * piece), "fb", 2, to_sib)
    take_x(tiles)
    arrive(rows_of(w1, far * shard + mine_at, SHARED * piece), "fb", 0, to_sib)
    arrive(rows_of(w1, far * shard + SHARED * piece, kept), "fb", 1, to_sib)
    arrive(rows_of(w1, far * shard + theirs_at, SHARED * piece), "fb", 2, to_sib)
    first = 2 + 3 * requests
    final(1, 0, first)
    final(1, 1, first + 1)
    take_x(1)
    arrive(att_all.at[peer], "yt", 0, to_peer)
    pass_on(att_all.at[peer], "ft", 0, to_sib)
    for r in range(2, requests - 1):
        final(1, r, first + r)
    take_x(1)
    project()
    take_x(1)
    final(1, requests - 1, first + requests - 1)
    while x_queue[0][0] == 0:
        take_x(1)
    take_y(2 * tiles)
    take_x(tiles)
    while y_queue[0][0] == 0:
        take_y(1)
    take_x(tiles)
    place_x(0)
    place_y(0)
    while len(x_queue) > tiles:
        take_x(1)
        take_y(1)
    take_x(1)
    take_y(1)
    total = terms[h]
    for k in range(1, heads):
        arrive(trecv.at[k - 1], "zt", k - 1, {"head": (h + heads - k) % heads})
        total = total + trecv[k - 1].astype(f32)
    decoded_ref[...] = total.astype(bf16)
    while x_queue:
        take_x(1)
    place_x(1)
    while y_queue:
        take_y(1)
    place_y(1)

    for ch in range(2):
        for r in range(requests):
            for i in range(tiles):
                remote(
                    half_block(hsend, ch * requests + r, i), half_block(recvx[ch], r, i),
                    "hx", (ch * requests + r) * tiles + i, to_x,
                ).wait_send()
    for copy in sent:
        copy.wait_send()
    for copy in placed[-OUTS:]:
        copy.wait()


def serve(
    prompt, key_value_weight, adapter_down_weight, adapter_up_weight, request_adapter_index,
    destination, rotated_query, key_value_cache, current_key_value, cached_length,
    row_adapter_index, output_weight, output_down_weight, output_up_weight,
):
    f32, bf16 = jnp.float32, jnp.bfloat16
    requests, tok, model = prompt.shape
    shard, _, width = key_value_weight.shape
    heads = lax.axis_size("head")
    members = lax.axis_size("seq")
    rows = rotated_query.shape[0]
    attn_width = rotated_query.shape[1]
    q_heads = attn_width // HEAD_DIM
    ranks = ADAPTER_COUNT * ADAPTER_RANK
    out_width = output_weight.shape[1]
    odown = output_down_weight.transpose(1, 2, 0).reshape(ranks, attn_width)
    oup = output_up_weight.reshape(ranks, out_width)
    slots = requests - 1
    ow_width = out_width // 4
    block = (2 * tok, PART)
    tiles = tok // TILE
    sems = 64 + 8 * requests * tiles
    vmem, smem, hbm = (
        pl.BlockSpec(memory_space=pltpu.VMEM),
        pl.BlockSpec(memory_space=pltpu.SMEM),
        pl.BlockSpec(memory_space=pl.ANY),
    )
    out, decoded = pl.pallas_call(
        serve_kernel,
        in_specs=[smem, smem, smem, hbm, hbm, hbm, hbm, hbm, hbm, hbm, vmem, hbm, hbm, hbm],
        out_specs=[hbm, vmem],
        out_shape=[
            jax.ShapeDtypeStruct((CAP, members, 2) + block, bf16),
            jax.ShapeDtypeStruct((rows, out_width), bf16),
        ],
        scratch_shapes=[
            pltpu.VMEM((model, 2 * PART), bf16),
            pltpu.VMEM((model, 2 * PART), bf16),
            pltpu.VMEM((2, shard, 2, PART), bf16),
            pltpu.VMEM((SLOTS, tok, 2 * shard), bf16),
            pltpu.VMEM((requests, tok, 2 * PART), f32),
            pltpu.VMEM(key_value_cache.shape, bf16),
            pltpu.VMEM((2, attn_width, ow_width), bf16),
            pltpu.VMEM(adapter_down_weight.shape, bf16),
            pltpu.VMEM(adapter_up_weight.shape, bf16),
            pltpu.VMEM(rotated_query.shape, bf16),
            pltpu.VMEM(current_key_value.shape, bf16),
            pltpu.VMEM(odown.shape, bf16),
            pltpu.VMEM(oup.shape, bf16),
            pltpu.VMEM((rows * q_heads, HEAD_DIM), f32),
            pltpu.VMEM((rows * q_heads, HEAD_DIM), f32),
            pltpu.VMEM((members, rows, attn_width), bf16),
            pltpu.VMEM((2 * ADAPTER_RANK, model), bf16),
            pltpu.VMEM((tok, 2 * ADAPTER_RANK), f32),
            pltpu.VMEM((requests, tiles, 2 * ADAPTER_RANK, TILE), bf16),
            pltpu.VMEM((requests, tok, PART), bf16),
            pltpu.VMEM((heads, rows, out_width), f32),
            pltpu.VMEM((heads - 1, rows, out_width), bf16),
            pltpu.VMEM((heads - 1, rows, out_width), bf16),
            pltpu.VMEM((2 * requests,) + block, bf16),
            pltpu.VMEM((OUTS, 2 * TILE, PART), bf16),
            pltpu.VMEM((requests,) + block, bf16),
            pltpu.VMEM((requests,) + block, bf16),
            pltpu.VMEM((requests,) + block, bf16),
            pltpu.VMEM((requests,) + block, bf16),
            pltpu.VMEM((2 * slots,) + block, bf16),
            pltpu.VMEM((slots,) + block, bf16),
            pltpu.VMEM((slots,) + block, bf16),
            pltpu.VMEM((slots,) + block, bf16),
            pltpu.VMEM((slots,) + block, bf16),
            pltpu.SemaphoreType.DMA((sems,)),
            pltpu.SemaphoreType.DMA((sems,)),
            pltpu.SemaphoreType.DMA((SLOTS + 11 + OUTS,)),
        ],
        compiler_params=pltpu.CompilerParams(
            collective_id=0, has_side_effects=True, vmem_limit_bytes=67043328
        ),
    )(
        destination, request_adapter_index, cached_length, prompt, key_value_weight, adapter_down_weight,
        adapter_up_weight, rotated_query, key_value_cache, current_key_value,
        row_adapter_index.reshape(1, -1), output_weight,
        odown, oup,
    )
    return join(out.reshape(CAP, members, 2, tok, 2, PART)), decoded


def join_kernel(in_ref, out_ref, buf, in_sem, out_sem):
    slots, members, halves, tok, _, lanes = in_ref.shape
    places = [(s, m, k) for s in range(slots) for m in range(members) for k in range(halves)]
    loads = [
        pltpu.make_async_copy(in_ref.at[place], buf.at[i], in_sem.at[i])
        for i, place in enumerate(places)
    ]
    for copy in loads:
        copy.start()
    stores = []
    for i, (s, m, k) in enumerate(places):
        loads[i].wait()
        copy = pltpu.make_async_copy(
            buf.at[i],
            out_ref.at[0, s, pl.ds(m * tok, tok), :, pl.ds(k * lanes, lanes)],
            out_sem.at[i],
        )
        copy.start()
        stores.append(copy)
    for copy in stores:
        copy.wait()


def join(blocks):
    slots, members, halves, tok, pair, lanes = blocks.shape
    count = slots * members * halves
    return pl.pallas_call(
        join_kernel,
        in_specs=[pl.BlockSpec(memory_space=pl.ANY)],
        out_specs=pl.BlockSpec(memory_space=pl.ANY),
        out_shape=jax.ShapeDtypeStruct((1, slots, members * tok, pair, halves * lanes), blocks.dtype),
        scratch_shapes=[
            pltpu.VMEM((count, tok, pair, lanes), blocks.dtype),
            pltpu.SemaphoreType.DMA((count,)),
            pltpu.SemaphoreType.DMA((count,)),
        ],
    )(blocks)


def fits(mesh):
    return mesh.shape["seq"] == 4 and mesh.shape["pool"] == 2


def solution(mesh):
    in_specs = (
        P("pool", "seq", None),
        P("seq", None, "head"),
        P("seq", None),
        P(None, None, None, "head"),
        P("pool"),
        P(),
        P(("pool", "seq"), "head"),
        P(("pool", "seq"), None, None, "head"),
        P(("pool", "seq"), None, "head"),
        P(("pool", "seq")),
        P("pool"),
        P("head", "seq"),
        P("head", None, None),
        P(None, None, "seq"),
    )
    out_specs = (P(("pool", "seq"), None, None, None, "head"), P(("pool", "head"), "seq"))
    run = serve if fits(mesh) else body
    return jax.shard_map(run, mesh=mesh, in_specs=in_specs, out_specs=out_specs, check_vma=False)
```

```python
import jax
import jax.numpy as jnp
from jax import lax
from jax.experimental import pallas as pl
from jax.experimental.pallas import tpu as pltpu
from jax.sharding import PartitionSpec as P

HEAD_DIM = 128
ADAPTER_RANK = 16
ADAPTER_COUNT = 8
CAP = 2


def exchanged(value, axis, mask):
    pairs = [(source, source ^ mask) for source in range(lax.axis_size(axis))]
    return lax.ppermute(value, axis, pairs)


def gathered(value, axis, after=None):
    size = lax.axis_size(axis)
    index = lax.axis_index(axis)
    held = value[None]
    mask = size // 2
    arrived = None
    while mask >= 1:
        other = exchanged(held, axis, mask)
        if after is not None:
            other = lax.optimization_barrier((other, after))[0]
        arrived = other if arrived is None else arrived
        low_bit = (index // mask) % 2 == 0
        first = jnp.where(low_bit, held, other)
        second = jnp.where(low_bit, other, held)
        held = jnp.stack([first, second], axis=1).reshape((-1,) + value.shape)
        mask //= 2
    return held, arrived


def scattered_sum(value, axis):
    size = lax.axis_size(axis)
    index = lax.axis_index(axis)
    held = value.reshape((size, value.shape[0] // size) + value.shape[1:])
    mask = 1
    while mask < size:
        split = held.reshape((held.shape[0] // 2, 2) + held.shape[1:])
        low_bit = (index // mask) % 2 == 0
        keep = jnp.where(low_bit, split[:, 0], split[:, 1])
        give = jnp.where(low_bit, split[:, 1], split[:, 0])
        held = keep + exchanged(give, axis, mask)
        mask *= 2
    return held[0]


def attend_kernel(lengths, query_ref, cache_ref, key_ref, value_ref, out_ref):
    rows, positions = cache_ref.shape[0], cache_ref.shape[1]
    kv_heads = key_ref.shape[1]
    groups = query_ref.shape[1] // kv_heads
    start = pl.program_id(0) * rows
    lane = lax.broadcasted_iota(jnp.int32, (groups, 2 * positions), 1)
    factor = HEAD_DIM ** (-0.5)
    blocks, scores, owns = [], [], []
    for row in range(rows):
        pairs = cache_ref[row].reshape(2 * positions, kv_heads * HEAD_DIM)
        valid = (lane % 2 == 0) & (lane < 2 * lengths[start + row])
        for head in range(kv_heads):
            block = pairs[:, head * HEAD_DIM : (head + 1) * HEAD_DIM]
            query = query_ref[row, head * groups : (head + 1) * groups, :]
            own_key = key_ref[row, head : head + 1, :].astype(jnp.float32)
            own = jnp.sum(query.astype(jnp.float32) * own_key, axis=1, keepdims=True) * factor
            score = lax.dot_general(
                query, block, (((1,), (1,)), ((), ())), preferred_element_type=jnp.float32
            )
            blocks.append(block)
            scores.append(jnp.where(valid, score * factor, -1e30))
            owns.append(own)
    scores = jnp.concatenate(scores, axis=0)
    own = jnp.concatenate(owns, axis=0)
    highest = jnp.maximum(jnp.max(scores, axis=1, keepdims=True), own)
    raw = jnp.where(scores > -1e29, jnp.exp(scores - highest), 0.0)
    own_raw = jnp.exp(own - highest)
    total = jnp.sum(raw, axis=1, keepdims=True) + own_raw
    weights = pltpu.roll(raw / total, 1, 1).astype(jnp.bfloat16)
    own_weight = (own_raw / total).astype(jnp.bfloat16).astype(jnp.float32)
    for row in range(rows):
        for head in range(kv_heads):
            at = (row * kv_heads + head) * groups
            own_value = value_ref[row, head : head + 1, :].astype(jnp.float32)
            mixed = jnp.dot(
                weights[at : at + groups],
                blocks[row * kv_heads + head],
                preferred_element_type=jnp.float32,
            )
            out_ref[row, head * groups : (head + 1) * groups, :] = (
                mixed + own_weight[at : at + groups] * own_value
            ).astype(jnp.bfloat16)


def attend(query, cache, current, lengths):
    rows, positions, _, width = cache.shape
    kv_heads = width // HEAD_DIM
    heads = query.shape[1] // HEAD_DIM
    step = next(size for size in (8, 4, 2, 1) if rows % size == 0)
    query = query.reshape(rows, heads, HEAD_DIM)
    own_key = current[:, 0].reshape(rows, kv_heads, HEAD_DIM)
    own_value = current[:, 1].reshape(rows, kv_heads, HEAD_DIM)
    out = pl.pallas_call(
        attend_kernel,
        grid_spec=pltpu.PrefetchScalarGridSpec(
            num_scalar_prefetch=1,
            grid=(rows // step,),
            in_specs=[
                pl.BlockSpec((step, heads, HEAD_DIM), lambda i, _: (i, 0, 0)),
                pl.BlockSpec((step, positions, 2, width), lambda i, _: (i, 0, 0, 0)),
                pl.BlockSpec((step, kv_heads, HEAD_DIM), lambda i, _: (i, 0, 0)),
                pl.BlockSpec((step, kv_heads, HEAD_DIM), lambda i, _: (i, 0, 0)),
            ],
            out_specs=pl.BlockSpec((step, heads, HEAD_DIM), lambda i, _: (i, 0, 0)),
        ),
        out_shape=jax.ShapeDtypeStruct((rows, heads, HEAD_DIM), jnp.bfloat16),
        cost_estimate=pl.CostEstimate(
            flops=8 * rows * heads * positions * HEAD_DIM,
            bytes_accessed=4 * rows * positions * width,
            transcendentals=2 * rows * heads * positions,
        ),
    )(lengths, query, cache, own_key, own_value)
    return out.reshape(rows, heads * HEAD_DIM)


def weave_kernel(key_ref, value_ref, out_ref):
    tokens, width = key_ref.shape[2], key_ref.shape[3]
    part = 128
    row = lax.broadcasted_iota(jnp.int32, (2 * part, 2 * part), 0)
    column = lax.broadcasted_iota(jnp.int32, (2 * part, 2 * part), 1)
    order = jnp.where(column == (row % 2) * part + row // 2, 1.0, 0.0).astype(jnp.bfloat16)
    for at in range(0, tokens, part):
        both = jnp.concatenate(
            [key_ref[0, 0, at : at + part, :], value_ref[0, 0, at : at + part, :]], axis=0
        )
        woven = jnp.dot(order, both, preferred_element_type=jnp.float32).astype(jnp.bfloat16)
        out_ref[0, 0, at : at + part, :, :] = woven.reshape(part, 2, width)


def weave(keys, values):
    sources, slots, tokens, width = keys.shape
    spec = pl.BlockSpec((1, 1, tokens, width), lambda slot, source: (source, slot, 0, 0))
    return pl.pallas_call(
        weave_kernel,
        grid=(slots, sources),
        in_specs=[spec, spec],
        out_specs=pl.BlockSpec(
            (1, 1, tokens, 2, width), lambda slot, source: (0, slot, source, 0, 0)
        ),
        out_shape=jax.ShapeDtypeStruct((1, slots, sources * tokens, 2, width), jnp.bfloat16),
        cost_estimate=pl.CostEstimate(
            flops=1024 * slots * sources * tokens * width,
            bytes_accessed=8 * slots * sources * tokens * width,
            transcendentals=0,
        ),
    )(keys, values)


def slot_hits(owners, decoders):
    requests = owners.shape[0]
    order = jnp.arange(requests, dtype=jnp.int32)
    same = owners[:, None] == owners[None, :]
    slot_of = jnp.sum((same & (order[None, :] < order[:, None])).astype(jnp.int32), axis=1)
    slot_hit = slot_of[None, :] == jnp.arange(CAP, dtype=jnp.int32)[:, None]
    owner_hit = owners[None, :] == jnp.arange(decoders, dtype=jnp.int32)[:, None]
    return owner_hit[:, None, :] & slot_hit[None, :, :]


def hand_over(arrived, hits, after):
    if after is not None:
        arrived = lax.optimization_barrier((arrived, after))[0]
    outgoing = jnp.zeros(hits.shape[:2] + arrived.shape[1:], arrived.dtype)
    for request in range(arrived.shape[0]):
        outgoing = jnp.where(
            hits[:, :, request][:, :, None, None], arrived[request][None, None], outgoing
        )
    landed = lax.all_to_all(outgoing, "seq", split_axis=0, concat_axis=0, tiled=True)
    return landed, outgoing


def body(
    prompt,
    key_value_weight,
    adapter_down_weight,
    adapter_up_weight,
    request_adapter_index,
    destination,
    rotated_query,
    key_value_cache,
    current_key_value,
    cached_length,
    row_adapter_index,
    output_weight,
    output_down_weight,
    output_up_weight,
):
    requests, tok_dev, model_width = prompt.shape
    width = key_value_weight.shape[2]
    shard = key_value_weight.shape[0]
    decoders = lax.axis_size("seq")
    heads = lax.axis_size("head")
    columns = 2 * ADAPTER_RANK
    tokens = prompt.reshape(requests * tok_dev, model_width)

    share = requests // heads if requests % heads == 0 else requests
    mine = lax.axis_index("head") * share if share < requests else 0
    my_adapter = lax.dynamic_slice_in_dim(request_adapter_index, mine, share)
    column = jnp.arange(ADAPTER_COUNT * columns, dtype=jnp.int32)
    wanted = my_adapter[:, None] * columns + jnp.arange(columns, dtype=jnp.int32)[None, :]
    pick = (wanted.reshape(-1)[:, None] == column[None, :]).astype(jnp.bfloat16)
    down = lax.dot_general(
        pick, adapter_down_weight, (((1,), (1,)), ((), ())), preferred_element_type=jnp.float32
    ).astype(jnp.bfloat16)
    matrix = key_value_weight.reshape(shard, 2 * width)
    down_all, down_first = gathered(down, "seq")
    matrix = lax.optimization_barrier((matrix, down_first))[0]
    key_all, key_first = gathered(matrix[:, :width], "seq")
    value_all, _ = gathered(matrix[:, width:], "seq", key_all)
    key_all = key_all.reshape(model_width, width)
    value_all = value_all.reshape(model_width, width)
    rotated_query = lax.optimization_barrier((rotated_query, key_first))[0]

    attended = attend(rotated_query, key_value_cache, current_key_value, cached_length)
    attn_rows = gathered(attended, "seq")[0].reshape(-1, attended.shape[1])
    ranks = ADAPTER_COUNT * ADAPTER_RANK
    down_flat = output_down_weight.reshape(output_down_weight.shape[0], ranks)
    up_flat = output_up_weight.reshape(ranks, output_up_weight.shape[2])
    rank_owner = jnp.arange(ranks, dtype=jnp.int32) // ADAPTER_RANK
    low_rows = jnp.dot(attn_rows, down_flat, preferred_element_type=jnp.float32)
    low_rows = jnp.where(row_adapter_index[:, None] == rank_owner[None, :], low_rows, 0.0)
    terms = jnp.dot(attn_rows, output_weight, preferred_element_type=jnp.float32)
    terms = terms + jnp.dot(
        low_rows.astype(jnp.bfloat16), up_flat, preferred_element_type=jnp.float32
    )
    decoded = scattered_sum(terms, "head").astype(jnp.bfloat16)

    my_tokens = lax.dynamic_slice_in_dim(prompt, mine, share, axis=0)
    my_down = down_all.transpose(1, 0, 2).reshape(share, columns, model_width)
    my_low = jnp.einsum("rtk,rck->rct", my_tokens, my_down, preferred_element_type=jnp.float32)
    low = gathered(my_low, "head")[0] if share < requests else my_low[None]
    low = low.reshape(requests, 2, ADAPTER_RANK, tok_dev).astype(jnp.bfloat16)
    own = jnp.eye(requests, dtype=jnp.bool_)[None, :, None, :, None]
    spread = jnp.where(
        own, low.transpose(1, 0, 2, 3)[:, :, :, None, :], jnp.zeros((), jnp.bfloat16)
    ).reshape(2, requests * ADAPTER_RANK, requests * tok_dev)
    selector = request_adapter_index[:, None] == jnp.arange(ADAPTER_COUNT, dtype=jnp.int32)[None, :]
    up = jnp.einsum(
        "um,mdzt->duzt",
        selector.astype(jnp.bfloat16),
        adapter_up_weight,
        preferred_element_type=jnp.float32,
    ).astype(jnp.bfloat16)
    up = up.reshape(2, requests * ADAPTER_RANK, width)

    pool_index = lax.axis_index("pool")
    other_owners = lax.dynamic_slice_in_dim(destination, (1 - pool_index) * requests, requests)
    hits = slot_hits(other_owners, decoders)

    arrived = []
    for which, weight in enumerate((key_all, value_all)):
        base = jnp.dot(tokens, weight, preferred_element_type=jnp.float32)
        extra = lax.dot_general(
            spread[which], up[which], (((0,), (0,)), ((), ())), preferred_element_type=jnp.float32
        )
        block = (base + extra).astype(jnp.bfloat16).reshape(requests, tok_dev, width)
        arrived.append(exchanged(block, "pool", 1))
    handed, outgoing = [], block
    for blocks in arrived:
        landed, outgoing = hand_over(blocks, hits, outgoing)
        handed.append(landed)
    return (weave(handed[0], handed[1]), decoded)


MESH = pl.DeviceIdType.MESH
PIECES = 8
SLOTS = 3
SHARED = 1
OUTS = 8
TILE = 256
PART = 128


def serve_kernel(
    dest_ref,
    adapter_ref,
    length_ref,
    prompt_ref,
    kv_ref,
    down_hbm,
    up_hbm,
    query_hbm,
    cache_ref,
    current_hbm,
    row_ref,
    ow_ref,
    odown_hbm,
    oup_hbm,
    out_ref,
    decoded_ref,
    w0,
    w1,
    kraw,
    pbuf,
    acc,
    cbuf,
    owbuf,
    down_ref,
    up_ref,
    query_ref,
    current_ref,
    odown_ref,
    oup_ref,
    qbuf,
    abuf,
    att_all,
    down_all,
    low_acc,
    low_flat,
    low_all,
    terms,
    tsend,
    trecv,
    decoded,
    hsend,
    stage,
    recvx0,
    recvx1,
    sibx0,
    sibx1,
    ysend,
    yrecv0,
    yrecv1,
    siby0,
    siby1,
    ssem,
    rsem,
    lsem,
):
    f32, bf16 = jnp.float32, jnp.bfloat16
    requests, tok, model = prompt_ref.shape
    shard = kv_ref.shape[0]
    half_width = 2 * shard
    heads = lax.axis_size("head")
    rows = query_ref.shape[0]
    q_heads = query_ref.shape[1] // HEAD_DIM
    columns = 2 * ADAPTER_RANK
    p, me, h = lax.axis_index("pool"), lax.axis_index("seq"), lax.axis_index("head")
    y, c = me // 2, me % 2
    sib, peer, far = y * 2 + 1 - c, (1 - y) * 2 + c, (1 - y) * 2 + 1 - c
    slots = requests - 1
    tiles = tok // TILE
    recvx, sibx = (recvx0, recvx1), (sibx0, sibx1)
    yrecv, siby = (yrecv0, yrecv1), (siby0, siby1)
    w = (w0, w1)

    names, at = {}, 0
    for name, count in (
        ("ya", PIECES), ("xa", PIECES), ("sa", 1), ("fa", 2 * PIECES),
        ("yb", SHARED + 1), ("xb", SHARED), ("sb", 1), ("fb", 3),
        ("yd", 1), ("sd", 1), ("fd", 1), ("yt", 1), ("st", 1), ("ft", 1),
        ("zl", heads - 1), ("zt", heads - 1),
        ("hx", 2 * requests * tiles + 1), ("hs", 2 * requests * tiles + 1),
        ("hy", 2 * slots * tiles + 1), ("hf", 2 * slots * tiles + 1),
    ):
        names[name] = at
        at += count

    sent = []

    def remote(src, dst, name, index, target):
        i = names[name] + index
        return pltpu.make_async_remote_copy(
            src_ref=src, dst_ref=dst, send_sem=ssem.at[i], recv_sem=rsem.at[i],
            device_id=target, device_id_type=MESH,
        )

    def send(src, dst, name, index, target):
        copy = remote(src, dst, name, index, target)
        copy.start()
        sent.append(copy)

    def arrive(dst, name, index, target):
        remote(dst, dst, name, index, target).wait_recv()

    to_sib, to_peer, to_x = {"seq": sib}, {"seq": peer}, {"pool": 1 - p}

    def rows_of(ref, start, size):
        return ref.at[pl.ds(pl.multiple_of(start, PART), size)]

    def pass_on(part, name, index, target):
        send(part, part, name, index, target)

    def kv_load(ch):
        return pltpu.make_async_copy(
            kv_ref.at[:, :, ch * PART : (ch + 1) * PART], kraw.at[ch], lsem.at[SLOTS + 1 + ch]
        )

    ends = SLOTS + 5 + OUTS
    small = [
        pltpu.make_async_copy(src, dst, lsem.at[ends + i])
        for i, (src, dst) in enumerate(
            (
                (down_hbm, down_ref), (up_hbm, up_ref), (query_hbm, query_ref),
                (current_hbm, current_ref), (odown_hbm, odown_ref), (oup_hbm, oup_ref),
            )
        )
    ]

    def prompt_load(step):
        if isinstance(step, int) and step < requests:
            r, half = step, y
        elif isinstance(step, int) and step < requests + 2:
            r, half = h, (y if step == requests else 1 - y)
        else:
            t = step - 2
            r, turn = t % requests, (t // requests) % 2
            half = turn + y - 2 * turn * y
        slot = step % SLOTS
        return pltpu.make_async_copy(
            prompt_ref.at[r, :, pl.ds(pl.multiple_of(half * half_width, half_width), half_width)],
            pbuf.at[slot],
            lsem.at[slot],
        )

    def ow_load(n):
        width = owbuf.shape[2]
        return pltpu.make_async_copy(
            ow_ref.at[:, pl.ds(pl.multiple_of(n * width, width), width)],
            owbuf.at[n % 2],
            lsem.at[SLOTS + 3 + n % 2],
        )

    total_steps = 2 + 4 * requests
    kv_load(0).start()
    small[0].start()

    barrier = pltpu.get_barrier_semaphore()
    partners = [to_sib, to_peer, to_x] + [{"head": (h + k) % heads} for k in range(1, heads)]
    for partner in partners:
        pl.semaphore_signal(barrier, inc=1, device_id=partner, device_id_type=MESH)
    prompt_load(0).start()
    kv_load(1).start()
    for step in range(1, SLOTS):
        prompt_load(step).start()
    for copy in small[1:]:
        copy.start()
    cache_copy = pltpu.make_async_copy(cache_ref, cbuf, lsem.at[SLOTS])
    cache_copy.start()
    ow_load(0).start()
    ow_load(1).start()

    order_row = lax.broadcasted_iota(jnp.int32, (2 * PART, 2 * PART), 0)
    order_col = lax.broadcasted_iota(jnp.int32, (2 * PART, 2 * PART), 1)
    order = jnp.where(order_col == (order_row % 2) * PART + order_row // 2, 1.0, 0.0).astype(bf16)
    unorder = jnp.where(order_row == (order_col % 2) * PART + order_col // 2, 1.0, 0.0).astype(bf16)

    def split_rows(ch, start, size):
        @pl.loop(0, size // PART)
        def _(b):
            row = pl.multiple_of(start + b * PART, PART)
            pairs = kraw[ch, pl.ds(row, PART)].reshape(2 * PART, PART)
            parts = jnp.dot(unorder, pairs, preferred_element_type=f32).astype(bf16)
            to = pl.ds(pl.multiple_of(me * shard + row, PART), PART)
            w[ch][to, :PART] = parts[:PART]
            w[ch][to, PART:] = parts[PART:]

    piece = shard // (2 * PIECES)
    half_shard = shard // 2

    def y_piece(k):
        pass_on(rows_of(w0, me * shard + (p * PIECES + k) * piece, piece), "ya", k, to_peer)

    def y_arrived(k):
        part = rows_of(w0, peer * shard + (p * PIECES + k) * piece, piece)
        arrive(part, "ya", k, to_peer)
        pass_on(part, "xa", k, to_x)
        pass_on(part, "fa", k, to_sib)

    def x_arrived(k):
        part = rows_of(w0, peer * shard + ((1 - p) * PIECES + k) * piece, piece)
        arrive(part, "xa", k, to_x)
        pass_on(part, "fa", PIECES + k, to_sib)

    def far_arrived():
        for k in range(PIECES):
            for turn, pool_part in enumerate((p, 1 - p)):
                part = rows_of(w0, far * shard + (pool_part * PIECES + k) * piece, piece)
                arrive(part, "fa", turn * PIECES + k, to_sib)

    kv_load(0).wait()
    split_rows(0, p * half_shard, half_shard)
    pl.semaphore_wait(barrier, len(partners))
    for k in range(PIECES // 2):
        y_piece(k)

    small[0].wait()
    pick_row = lax.broadcasted_iota(jnp.int32, (columns, down_ref.shape[1]), 0)
    pick_col = lax.broadcasted_iota(jnp.int32, (columns, down_ref.shape[1]), 1)
    pick = jnp.where(pick_col == pick_row + adapter_ref[h] * columns, 1.0, 0.0).astype(bf16)

    def cols_at(who):
        return down_all.at[:, pl.ds(pl.multiple_of(who * shard, shard), shard)]

    down_all[:, pl.ds(pl.multiple_of(me * shard, shard), shard)] = lax.dot_general(
        pick, down_ref[...], (((1,), (1,)), ((), ())), preferred_element_type=f32
    ).astype(bf16)
    split_rows(0, (1 - p) * half_shard, half_shard)
    pass_on(cols_at(me), "yd", 0, to_peer)
    pass_on(cols_at(me), "sd", 0, to_sib)
    for k in range(PIECES // 2, PIECES):
        y_piece(k)
    pass_on(rows_of(w0, me * shard, shard), "sa", 0, to_sib)

    def base(ch, r, step):
        prompt_load(step).wait()

        @pl.loop(0, tiles)
        def _(i):
            at_row = pl.ds(pl.multiple_of(i * TILE, TILE), TILE)
            weight = w[ch][pl.ds(pl.multiple_of(y * half_width, half_width), half_width), :]
            acc[r, at_row, :] = jnp.dot(
                pbuf[step % SLOTS, at_row, :], weight, preferred_element_type=f32
            )

        prompt_load(step + SLOTS).start()

    kv_load(1).wait()
    kept = shard - 2 * SHARED * piece
    mine_at = p * (shard - SHARED * piece)
    theirs_at = (1 - p) * (shard - SHARED * piece)
    if SHARED:
        split_rows(1, mine_at, SHARED * piece)
    for k in range(SHARED):
        pass_on(rows_of(w1, me * shard + mine_at + k * piece, piece), "yb", k, to_peer)
    split_rows(1, SHARED * piece, kept)
    pass_on(rows_of(w1, me * shard + SHARED * piece, kept), "yb", SHARED, to_peer)
    if SHARED:
        split_rows(1, theirs_at, SHARED * piece)

    arrive(rows_of(w0, sib * shard, shard), "sa", 0, to_sib)
    for k in range(PIECES // 2 - 1):
        y_arrived(k)
    base(0, 0, 0)
    y_arrived(PIECES // 2 - 1)
    base(0, 1, 1)
    base(0, 2, 2)
    arrive(cols_at(peer), "yd", 0, to_peer)
    pass_on(cols_at(peer), "fd", 0, to_sib)
    for r in range(3, requests):
        base(0, r, r)
    y_arrived(PIECES // 2)

    pass_on(rows_of(w1, me * shard, shard), "sb", 0, to_sib)
    arrive(cols_at(sib), "sd", 0, to_sib)
    arrive(cols_at(far), "fd", 0, to_sib)

    for turn in range(2):
        y_arrived(PIECES // 2 + 1 + turn)
        step = requests + turn
        prompt_load(step).wait()
        half = y if turn == 0 else 1 - y
        cols = pl.ds(pl.multiple_of(half * half_width, half_width), half_width)

        @pl.loop(0, tiles)
        def _(i):
            at_row = pl.ds(pl.multiple_of(i * TILE, TILE), TILE)
            part = lax.dot_general(
                pbuf[step % SLOTS, at_row, :], down_all[:, cols], (((1,), (1,)), ((), ())),
                preferred_element_type=f32,
            )
            if turn == 0:
                low_acc[at_row, :] = part
            else:
                low = jnp.concatenate(
                    [low_acc[at_row, :] + part, jnp.zeros((TILE, PART - columns), f32)], axis=1
                )
                low_flat[h, i] = low.T[:columns].astype(bf16)

        prompt_load(step + SLOTS).start()
    for k in range(1, heads):
        pass_on(low_flat.at[h], "zl", k - 1, {"head": (h + k) % heads})
    for k in range(PIECES // 2 + 3, PIECES):
        y_arrived(k)
    for copy in small[1:]:
        copy.wait()

    def spans(ch, r):
        if ch == 1 and r == requests - 1:
            ends_at = [0] + [(i + 1) * TILE for i in range(tiles - 1)] + [tok - PART, tok]
        else:
            ends_at = [i * TILE for i in range(tiles + 1)]
        return [(2 * a, 2 * (b - a)) for a, b in zip(ends_at, ends_at[1:])]

    def part_of(ref, index, span):
        return ref.at[index, pl.ds(span[0], span[1])]

    def sem_at(ch, r, i):
        return (ch * requests + r) * tiles + i

    def final(ch, r, step):
        lanes = slice(ch * PART, (ch + 1) * PART)
        prompt_load(step).wait()
        adapter = adapter_ref[r]
        up_key, up_value = up_ref[adapter, 0][:, lanes], up_ref[adapter, 1][:, lanes]
        gap = jnp.zeros_like(up_key)
        up = jnp.concatenate(
            [
                jnp.concatenate([up_key, gap], axis=1),
                jnp.concatenate([gap, up_value], axis=1),
                jnp.zeros((PART - columns, 2 * PART), bf16),
            ],
            axis=0,
        )

        @pl.loop(0, tiles)
        def _(i):
            at_row = pl.ds(pl.multiple_of(i * TILE, TILE), TILE)
            weight = w[ch][
                pl.ds(pl.multiple_of((1 - y) * half_width, half_width), half_width), :
            ]
            value = (
                acc[r, at_row, :]
                + jnp.dot(pbuf[step % SLOTS, at_row, :], weight, preferred_element_type=f32)
                + jnp.dot(low_all[r, at_row, :], up, preferred_element_type=f32)
            ).astype(bf16)
            for sub in range(TILE // PART):
                x = value[sub * PART : (sub + 1) * PART]
                both = jnp.concatenate([x[:, :PART], x[:, PART:]], axis=0)
                woven = jnp.dot(order, both, preferred_element_type=f32).astype(bf16)
                hsend[
                    ch * requests + r,
                    pl.ds(pl.multiple_of(2 * (i * TILE + sub * PART), 2 * PART), 2 * PART), :,
                ] = woven
            if (ch, r) != (1, requests - 1):
                span = (pl.multiple_of(i * 2 * TILE, 2 * TILE), 2 * TILE)
                remote(
                    part_of(hsend, ch * requests + r, span), part_of(recvx[ch], r, span),
                    "hx", sem_at(ch, r, i), to_x,
                ).start()

        if (ch, r) == (1, requests - 1):
            for i, span in enumerate(spans(ch, r)):
                remote(
                    part_of(hsend, ch * requests + r, span), part_of(recvx[ch], r, span),
                    "hx", sem_at(ch, r, i), to_x,
                ).start()
        if step + SLOTS < total_steps:
            prompt_load(step + SLOTS).start()

    for head in range(q_heads):
        qbuf[pl.ds(head, rows, stride=q_heads), :] = query_ref[
            :, head * HEAD_DIM : (head + 1) * HEAD_DIM
        ].astype(f32)
    cache_copy.wait()
    positions = cache_ref.shape[1]
    kv_heads = current_ref.shape[2] // HEAD_DIM
    groups = q_heads // kv_heads
    batch = 8
    factor = HEAD_DIM ** (-0.5)
    lane = lax.broadcasted_iota(jnp.int32, (groups, 2 * positions), 1)

    batches = rows // batch

    def attend_step(step):
        start = step * batch
        blocks, scores, owns, values = [], [], [], []
        for row in range(batch):
            pairs = cbuf[start + row].reshape(2 * positions, kv_heads * HEAD_DIM)
            valid = (lane % 2 == 0) & (lane < 2 * length_ref[start + row])
            now = current_ref[start + row].astype(f32)
            for head in range(kv_heads):
                span = slice(head * HEAD_DIM, (head + 1) * HEAD_DIM)
                block = pairs[:, span]
                query = qbuf[
                    pl.ds(pl.multiple_of((start + row) * q_heads + head * groups, groups), groups), :
                ]
                own = jnp.sum(query * now[0:1, span], axis=1, keepdims=True) * factor
                score = lax.dot_general(
                    query.astype(bf16), block, (((1,), (1,)), ((), ())), preferred_element_type=f32
                )
                blocks.append(block)
                scores.append(jnp.where(valid, score * factor, -1e30))
                owns.append(own)
                values.append(now[1:2, span])
        score = jnp.concatenate(scores, axis=0)
        own = jnp.concatenate(owns, axis=0)
        highest = jnp.maximum(jnp.max(score, axis=1, keepdims=True), own)
        raw = jnp.where(score > -1e29, jnp.exp(score - highest), 0.0)
        own_raw = jnp.exp(own - highest)
        normer = jnp.sum(raw, axis=1, keepdims=True) + own_raw
        weights = pltpu.roll(raw / normer, 1, 1).astype(bf16)
        own_weight = (own_raw / normer).astype(bf16).astype(f32)
        for item in range(batch * kv_heads):
            at_row = item * groups
            mixed = jnp.dot(
                weights[at_row : at_row + groups], blocks[item], preferred_element_type=f32
            )
            abuf[
                pl.ds(pl.multiple_of(start * q_heads + at_row, groups), groups), :
            ] = mixed + own_weight[at_row : at_row + groups] * values[item]

    def attend(start, stop):
        pl.loop(start, stop)(attend_step)

    for k in range(PIECES // 2):
        x_arrived(k)
    attend(0, batches // 3)
    for k in range(PIECES // 2, PIECES - 1):
        x_arrived(k)
    x_arrived(PIECES - 1)
    attend(batches // 3, batches // 2)
    for k in range(1, heads):
        source = (h + heads - k) % heads
        arrive(low_flat.at[source], "zl", k - 1, {"head": source})

    @pl.loop(0, requests)
    def _(r):
        for i in range(tiles):
            low = jnp.concatenate(
                [low_flat[r, i].astype(f32), jnp.zeros((PART - columns, TILE), f32)], axis=0
            )
            low_all[r, i * TILE : (i + 1) * TILE, :] = low.T.astype(bf16)

    far_arrived()

    def shared_arrived(k):
        part = rows_of(w1, peer * shard + mine_at + k * piece, piece)
        arrive(part, "yb", k, to_peer)
        pass_on(part, "xb", k, to_x)

    first = 2 + requests
    for r in range(requests):
        final(0, r, first + r)
        if r < SHARED:
            shared_arrived(r)
    if SHARED:
        pass_on(rows_of(w1, peer * shard + mine_at, SHARED * piece), "fb", 0, to_sib)

    attend(batches // 2, batches)
    for head in range(q_heads):
        att_all[me, :, head * HEAD_DIM : (head + 1) * HEAD_DIM] = abuf[
            pl.ds(head, rows, stride=q_heads), :
        ].astype(bf16)
    pass_on(att_all.at[me], "yt", 0, to_peer)
    pass_on(att_all.at[me], "st", 0, to_sib)

    other = (1 - p) * requests
    owner = [dest_ref[other + r] for r in range(requests)]
    away = [jnp.where(owner[r] // 2 == y, 0, 1) for r in range(requests)]

    def some(flags):
        kept = flags[0]
        for flag in flags[1:]:
            kept = jnp.maximum(kept, flag)
        return kept

    chosen = []
    for s in range(CAP):
        index, found, slot = 0, 0, 0
        for r in range(requests):
            before = sum([jnp.where(owner[q] == owner[r], 1, 0) for q in range(r)], 0)
            hit = jnp.where((owner[r] == me) & (before == s), 1, 0)
            shift = some(away[:r]) if r > 0 else 0
            index, found, slot = index + hit * r, found + hit, slot + hit * (r - shift)
        chosen.append((found, index, jnp.clip(slot, 0, slots - 1)))

    def on_x(ch, r, i):
        span = spans(ch, r)[i]
        part = part_of(recvx[ch], r, span)
        arrive(part, "hx", sem_at(ch, r, i), to_x)
        send(part, part_of(sibx[ch], r, span), "hs", sem_at(ch, r, i), to_sib)
        if r >= 1:
            j, k = r - 1, sem_at(ch, r - 1, i) - ch * tiles
            at_row = slice(span[0], span[0] + span[1])
            late = jnp.full((1, 1), some([1 - a for a in away[: j + 1]]), jnp.int32) > 0
            ysend[ch * slots + j, at_row] = jnp.where(
                late, recvx[ch][r, at_row], recvx[ch][j, at_row]
            )
            send(
                part_of(ysend, ch * slots + j, span), part_of(yrecv[ch], j, span), "hy", k, to_peer
            )

    def on_y(ch, j, i):
        span = spans(ch, j + 1)[i]
        part, k = part_of(yrecv[ch], j, span), sem_at(ch, j, i) - ch * tiles
        arrive(part, "hy", k, to_peer)
        send(part, part_of(siby[ch], j, span), "hf", k, to_sib)

    placed = []

    def place(ch, source, ref, by_slot, i):
        span = pl.ds(i * 2 * TILE, 2 * TILE)
        for s, (found, index, slot) in enumerate(chosen):
            got = jnp.full((1, 1), found, jnp.int32) > 0
            value = ref[slot if by_slot else index, span]
            turn = len(placed)
            if turn >= OUTS:
                placed[turn - OUTS].wait()
            stage[turn % OUTS] = jnp.where(got, value, jnp.zeros_like(value))
            copy = pltpu.make_async_copy(
                stage.at[turn % OUTS], out_ref.at[s, source, ch, span],
                lsem.at[SLOTS + 5 + turn % OUTS],
            )
            copy.start()
            placed.append(copy)

    def place_x(ch):
        for i in range(tiles):
            place(ch, me, recvx[ch], False, i)
        for r in range(requests):
            for i, span in enumerate(spans(ch, r)):
                arrive(part_of(sibx[ch], r, span), "hs", sem_at(ch, r, i), to_sib)
        for i in range(tiles):
            place(ch, sib, sibx[ch], False, i)

    def place_y(ch):
        for i in range(tiles):
            place(ch, peer, yrecv[ch], True, i)
        for j in range(slots):
            for i, span in enumerate(spans(ch, j + 1)):
                arrive(part_of(siby[ch], j, span), "hf", sem_at(ch, j, i) - ch * tiles, to_sib)
        for i in range(tiles):
            place(ch, far, siby[ch], True, i)

    x_queue = [
        (ch, r, i) for ch in range(2) for r in range(requests) for i in range(len(spans(ch, r)))
    ]
    y_queue = [
        (ch, j, i) for ch in range(2) for j in range(slots) for i in range(len(spans(ch, j + 1)))
    ]

    def take_x(count):
        for _ in range(count):
            on_x(*x_queue.pop(0))

    def take_y(count):
        for _ in range(count):
            on_y(*y_queue.pop(0))

    def project():
        arrive(att_all.at[sib], "st", 0, to_sib)
        arrive(att_all.at[far], "ft", 0, to_sib)
        members = att_all.shape[0]
        low_rows = lax.dot_general(
            odown_ref[...], att_all[...].reshape(members * rows, q_heads * HEAD_DIM),
            (((1,), (1,)), ((), ())), preferred_element_type=f32,
        )
        rank_owner = lax.broadcasted_iota(jnp.int32, low_rows.shape, 0) // ADAPTER_RANK
        low_rows = jnp.where(rank_owner == row_ref[...], low_rows, 0.0).astype(bf16)
        ow_width = owbuf.shape[2]
        blocks = ow_ref.shape[1] // ow_width

        def step(n):
            ow_load(n).wait()
            cols = pl.ds(pl.multiple_of(n * ow_width, ow_width), ow_width)
            part = jnp.dot(
                att_all[...].reshape(members * rows, q_heads * HEAD_DIM), owbuf[n % 2],
                preferred_element_type=f32,
            ) + lax.dot_general(
                low_rows, oup_ref[:, cols], (((0,), (0,)), ((), ())), preferred_element_type=f32
            )
            terms[:, :, cols] = part.reshape(heads, rows, ow_width)

            @pl.when(n + 2 < blocks)
            def _():
                ow_load(n + 2).start()

        pl.loop(0, blocks // 2)(step)
        take_x(1)
        pl.loop(blocks // 2, blocks)(step)

        for k in range(1, heads):
            target = (h + k) % heads
            tsend[k - 1] = terms[target].astype(bf16)
            send(tsend.at[k - 1], trecv.at[k - 1], "zt", k - 1, {"head": target})

    take_x(tiles)
    for k in range(SHARED):
        arrive(rows_of(w1, peer * shard + theirs_at + k * piece, piece), "xb", k, to_x)
    if SHARED:
        pass_on(rows_of(w1, peer * shard + theirs_at, SHARED * piece), "fb", 2, to_sib)
    arrive(rows_of(w1, sib * shard, shard), "sb", 0, to_sib)
    first = 2 + 2 * requests
    for r in range(requests):
        base(1, r, first + r)
        if r == requests - 2:
            part = rows_of(w1, peer * shard + SHARED * piece, kept)
            arrive(part, "yb", SHARED, to_peer)
            pass_on(part, "fb", 1, to_sib)
            take_x(1)
    take_x(tiles - 1)
    if SHARED:
        arrive(rows_of(w1, far * shard + mine_at, SHARED * piece), "fb", 0, to_sib)
        arrive(rows_of(w1, far * shard + theirs_at, SHARED * piece), "fb", 2, to_sib)
    arrive(rows_of(w1, far * shard + SHARED * piece, kept), "fb", 1, to_sib)
    first = 2 + 3 * requests
    final(1, 0, first)
    take_x(1)
    final(1, 1, first + 1)
    take_x(1)
    arrive(att_all.at[peer], "yt", 0, to_peer)
    pass_on(att_all.at[peer], "ft", 0, to_sib)
    for r in range(2, requests - 1):
        final(1, r, first + r)
        take_x(1)
    project()
    final(1, requests - 1, first + requests - 1)
    while x_queue[0][0] == 0:
        take_x(1)

    take_x(tiles)
    for i in range(tiles):
        while len([item for item in y_queue if item[0] == 0]) > tiles - i:
            take_y(1)
        take_x(1)
    while y_queue[0][0] == 0:
        take_y(1)
    place_x(0)
    place_y(0)
    for r in range(2, requests - 1):
        take_x(tiles)
        take_y(tiles)
    take_x(1)
    take_y(1)
    while x_queue:
        take_x(1)
    total = terms[h]
    for k in range(1, heads):
        arrive(trecv.at[k - 1], "zt", k - 1, {"head": (h + heads - k) % heads})
        total = total + trecv[k - 1].astype(f32)
    decoded[...] = total.astype(bf16)
    decoded_copy = pltpu.make_async_copy(decoded, decoded_ref, lsem.at[ends + len(small)])
    decoded_copy.start()
    place_x(1)
    while y_queue:
        take_y(1)
    place_y(1)

    for ch in range(2):
        for r in range(requests):
            for i, span in enumerate(spans(ch, r)):
                remote(
                    part_of(hsend, ch * requests + r, span), part_of(recvx[ch], r, span),
                    "hx", sem_at(ch, r, i), to_x,
                ).wait_send()
    for copy in sent:
        copy.wait_send()
    for copy in placed[-OUTS:]:
        copy.wait()
    decoded_copy.wait()


def serve(
    prompt, key_value_weight, adapter_down_weight, adapter_up_weight, request_adapter_index,
    destination, rotated_query, key_value_cache, current_key_value, cached_length,
    row_adapter_index, output_weight, output_down_weight, output_up_weight,
):
    f32, bf16 = jnp.float32, jnp.bfloat16
    requests, tok, model = prompt.shape
    shard, _, width = key_value_weight.shape
    heads = lax.axis_size("head")
    members = lax.axis_size("seq")
    rows = rotated_query.shape[0]
    attn_width = rotated_query.shape[1]
    q_heads = attn_width // HEAD_DIM
    ranks = ADAPTER_COUNT * ADAPTER_RANK
    out_width = output_weight.shape[1]
    odown = output_down_weight.transpose(1, 2, 0).reshape(ranks, attn_width)
    oup = output_up_weight.reshape(ranks, out_width)
    slots = requests - 1
    ow_width = out_width // 4
    block = (2 * tok, PART)
    tiles = tok // TILE
    sems = 96 + 8 * requests * tiles
    vmem, smem, hbm = (
        pl.BlockSpec(memory_space=pltpu.VMEM),
        pl.BlockSpec(memory_space=pltpu.SMEM),
        pl.BlockSpec(memory_space=pl.ANY),
    )
    out, decoded = pl.pallas_call(
        serve_kernel,
        in_specs=[smem, smem, smem, hbm, hbm, hbm, hbm, hbm, hbm, hbm, vmem, hbm, hbm, hbm],
        out_specs=[hbm, hbm],
        out_shape=[
            jax.ShapeDtypeStruct((CAP, members, 2) + block, bf16),
            jax.ShapeDtypeStruct((rows, out_width), bf16),
        ],
        scratch_shapes=[
            pltpu.VMEM((model, 2 * PART), bf16),
            pltpu.VMEM((model, 2 * PART), bf16),
            pltpu.VMEM((2, shard, 2, PART), bf16),
            pltpu.VMEM((SLOTS, tok, 2 * shard), bf16),
            pltpu.VMEM((requests, tok, 2 * PART), f32),
            pltpu.VMEM(key_value_cache.shape, bf16),
            pltpu.VMEM((2, attn_width, ow_width), bf16),
            pltpu.VMEM(adapter_down_weight.shape, bf16),
            pltpu.VMEM(adapter_up_weight.shape, bf16),
            pltpu.VMEM(rotated_query.shape, bf16),
            pltpu.VMEM(current_key_value.shape, bf16),
            pltpu.VMEM(odown.shape, bf16),
            pltpu.VMEM(oup.shape, bf16),
            pltpu.VMEM((rows * q_heads, HEAD_DIM), f32),
            pltpu.VMEM((rows * q_heads, HEAD_DIM), f32),
            pltpu.VMEM((members, rows, attn_width), bf16),
            pltpu.VMEM((2 * ADAPTER_RANK, model), bf16),
            pltpu.VMEM((tok, 2 * ADAPTER_RANK), f32),
            pltpu.VMEM((requests, tiles, 2 * ADAPTER_RANK, TILE), bf16),
            pltpu.VMEM((requests, tok, PART), bf16),
            pltpu.VMEM((heads, rows, out_width), f32),
            pltpu.VMEM((heads - 1, rows, out_width), bf16),
            pltpu.VMEM((heads - 1, rows, out_width), bf16),
            pltpu.VMEM((rows, out_width), bf16),
            pltpu.VMEM((2 * requests,) + block, bf16),
            pltpu.VMEM((OUTS, 2 * TILE, PART), bf16),
            pltpu.VMEM((requests,) + block, bf16),
            pltpu.VMEM((requests,) + block, bf16),
            pltpu.VMEM((requests,) + block, bf16),
            pltpu.VMEM((requests,) + block, bf16),
            pltpu.VMEM((2 * slots,) + block, bf16),
            pltpu.VMEM((slots,) + block, bf16),
            pltpu.VMEM((slots,) + block, bf16),
            pltpu.VMEM((slots,) + block, bf16),
            pltpu.VMEM((slots,) + block, bf16),
            pltpu.SemaphoreType.DMA((sems,)),
            pltpu.SemaphoreType.DMA((sems,)),
            pltpu.SemaphoreType.DMA((SLOTS + 12 + OUTS,)),
        ],
        compiler_params=pltpu.CompilerParams(
            collective_id=0, has_side_effects=True, vmem_limit_bytes=67043328
        ),
    )(
        destination, request_adapter_index, cached_length, prompt, key_value_weight, adapter_down_weight,
        adapter_up_weight, rotated_query, key_value_cache, current_key_value,
        row_adapter_index.reshape(1, -1), output_weight,
        odown, oup,
    )
    return join(out.reshape(CAP, members, 2, tok, 2, PART)), decoded


def join_kernel(in_ref, out_ref, buf, in_sem, out_sem):
    slots, members, halves, tok, _, lanes = in_ref.shape
    places = [(s, m, k) for s in range(slots) for m in range(members) for k in range(halves)]
    loads = [
        pltpu.make_async_copy(in_ref.at[place], buf.at[i], in_sem.at[i])
        for i, place in enumerate(places)
    ]
    for copy in loads:
        copy.start()
    stores = []
    for i, (s, m, k) in enumerate(places):
        loads[i].wait()
        copy = pltpu.make_async_copy(
            buf.at[i],
            out_ref.at[0, s, pl.ds(m * tok, tok), :, pl.ds(k * lanes, lanes)],
            out_sem.at[i],
        )
        copy.start()
        stores.append(copy)
    for copy in stores:
        copy.wait()


def join(blocks):
    slots, members, halves, tok, pair, lanes = blocks.shape
    count = slots * members * halves
    return pl.pallas_call(
        join_kernel,
        in_specs=[pl.BlockSpec(memory_space=pl.ANY)],
        out_specs=pl.BlockSpec(memory_space=pl.ANY),
        out_shape=jax.ShapeDtypeStruct((1, slots, members * tok, pair, halves * lanes), blocks.dtype),
        scratch_shapes=[
            pltpu.VMEM((count, tok, pair, lanes), blocks.dtype),
            pltpu.SemaphoreType.DMA((count,)),
            pltpu.SemaphoreType.DMA((count,)),
        ],
    )(blocks)


def fits(mesh):
    return mesh.shape["seq"] == 4 and mesh.shape["pool"] == 2


def solution(mesh):
    in_specs = (
        P("pool", "seq", None),
        P("seq", None, "head"),
        P("seq", None),
        P(None, None, None, "head"),
        P("pool"),
        P(),
        P(("pool", "seq"), "head"),
        P(("pool", "seq"), None, None, "head"),
        P(("pool", "seq"), None, "head"),
        P(("pool", "seq")),
        P("pool"),
        P("head", "seq"),
        P("head", None, None),
        P(None, None, "seq"),
    )
    out_specs = (P(("pool", "seq"), None, None, None, "head"), P(("pool", "head"), "seq"))
    run = serve if fits(mesh) else body
    return jax.shard_map(run, mesh=mesh, in_specs=in_specs, out_specs=out_specs, check_vma=False)
```
